32 devices in a mesh: gx: 8 (over z, x), gy: 4 (over y, core).
Axes of the slice: x: 2, y: 2, z: 4, core: 2. Of those that a mesh axis runs over, the one named last changes fastest.
Arguments:
- mode_fields: float32 [32, 512, 1024], P(None, 'gx', 'gy'), may hold values from -60 to 60, as said below
- conductance: float32 [512, 1024], P('gx', 'gy'), may hold values from 0.5 to 2
- potential: float32 [512, 1024], P('gx', 'gy'), may hold values from 0.25 to 4
Outputs:
- basis_field: float32 [128, 512, 1024], P(None, 'gx', 'gy')
- scaled_factor: float32 [128, 128], replicated
The draws below stay inside these ranges and needn't reach their ends.
Inputs may be any that keep to these rules, and one draw needn't show every extreme that they name: `mode_fields`: Real-valued mode amplitudes.
All inputs are finite; a program needn't handle non-finite values.
Results may differ from the reference program's by a relative error of at most 0.0003.
Values sent between devices are 32-bit elements; how exact they have to be, the bound alone decides.
A program may use at most 64 MiB of HBM per device.

```python
import math
import jax
import jax.numpy as jnp
from jax import lax

K = 32
C = 128
CX = 64
NX = 512
NY = 1024


def draw_mode_fields(key, part):
    key_scale, key_noise = jax.random.split(key, 2)
    col_scale = 10.0 ** jax.random.uniform(key_scale, (K, 1, 1), jnp.float32, -0.5, 0.5)
    row_pos = jnp.arange(NX, dtype=jnp.float32) / max(NX - 1, 1)
    row_scale = (10.0 ** (row_pos - 0.5))[None, :, None]
    noise = jax.random.truncated_normal(key_noise, -6.0, 6.0, (K, NX, NY), jnp.float32)
    return (col_scale * row_scale * noise).astype(jnp.float32)


def levels(own_key, dims, cuts, smallest, largest):
    def one(axis_at, shards_of):
        draws = jax.random.uniform(jax.random.fold_in(jax.random.fold_in(own_key, 6), axis_at), (shards_of,), jnp.float32, smallest / len(cuts), largest / len(cuts))
        return jnp.repeat(jnp.exp(draws), dims[axis_at] // shards_of).reshape((-1,) + (1,) * (len(dims) - axis_at - 1))

    loudness = one(*cuts[0])
    for cut in cuts[1:]:
        loudness = loudness * one(*cut)
    return loudness


def setup_inputs(seed: int = 0) -> dict:
    key_list = jax.random.split(jax.random.key(seed), 4)
    mode_fields = draw_mode_fields(jax.random.fold_in(key_list[3], 71), 0)
    conductance = jnp.clip(jnp.exp(math.log(2.0) - 1.3862944 * jax.random.uniform(key_list[1], (NX, NY), jnp.float32) ** levels(key_list[1], (NX, NY), ((0, 8), (1, 4)), -0.2, 0.2)), 0.5, 2.0)
    potential = jnp.clip(jnp.exp(math.log(4.0) - 2.7725887 * jax.random.uniform(key_list[2], (NX, NY), jnp.float32) ** levels(key_list[2], (NX, NY), ((0, 8), (1, 4)), -0.2, 0.2)), 0.25, 4.0)
    return {"mode_fields": mode_fields, "conductance": conductance, "potential": potential}


def build_columns(fields, conduct, potential):
    center = fields[:, 1:-1, 1:-1]
    k_mid = conduct[1:-1, 1:-1]
    x_plus = 0.5 * (k_mid + conduct[2:, 1:-1])
    x_minus = 0.5 * (k_mid + conduct[:-2, 1:-1])
    y_plus = 0.5 * (k_mid + conduct[1:-1, 2:])
    y_minus = 0.5 * (k_mid + conduct[1:-1, :-2])
    along_x = x_plus * (center - fields[:, 2:, 1:-1]) + x_minus * (center - fields[:, :-2, 1:-1])
    along_y = y_plus * (center - fields[:, 1:-1, 2:]) + y_minus * (center - fields[:, 1:-1, :-2])
    react = potential * center
    stacked = jnp.concatenate([center, along_x, along_y, react], 0)
    return stacked.reshape(stacked.shape[0], -1)

def reference(mode_fields, conductance, potential):
    pad_u = jnp.pad(mode_fields, ((0, 0), (1, 1), (1, 1)))
    pad_k = jnp.pad(conductance, 1)
    strips = NX // CX
    cell_count = float(NX * NY)

    def strip_columns(index):
        start = (index * CX).astype(jnp.int32)
        fields = lax.dynamic_slice_in_dim(pad_u, start, CX + 2, 1)
        conduct = lax.dynamic_slice_in_dim(pad_k, start, CX + 2, 0)
        react = lax.dynamic_slice_in_dim(potential, start, CX, 0)
        return build_columns(fields, conduct, react)

    def add_gram(carry, index):
        matrix = strip_columns(index)
        return (carry + jnp.dot(matrix, matrix.T, precision=lax.Precision.HIGHEST), None)
    indices = jnp.arange(strips, dtype=jnp.int32)
    gram_total, _ = lax.scan(add_gram, jnp.zeros((C, C), jnp.float32), indices)
    lower_tri = jnp.linalg.cholesky(gram_total / cell_count)

    def solve_strip(index):
        solved = jax.scipy.linalg.solve_triangular(lower_tri, strip_columns(index), lower=True)
        return solved.reshape(C, CX, NY)
    blocks = lax.map(solve_strip, indices)
    basis_field = blocks.transpose(1, 0, 2, 3).reshape(C, NX, NY)
    return (basis_field, lower_tri.T)
```

```python
import functools

import jax
import jax.numpy as jnp
from jax import lax
from jax.experimental import pallas as pl
from jax.experimental.pallas import tpu as pltpu
from jax.sharding import PartitionSpec as P

MESH = pl.DeviceIdType.MESH
F32 = jnp.float32
BF16 = jnp.bfloat16


def split(value):
    high = value.astype(BF16)
    return high, (value - high.astype(F32)).astype(BF16)


def gram_kernel(
    nx, ny, u_hbm, k_hbm, p_hbm, m_ref, g_ref,
    wide, kappa, p_ref, xface, yface, yleft, edge, halo, kside, acc, part, piece, ring, full,
    load, halo_send, halo_recv, rs_send, rs_recv, all_send, all_recv, ag_send, ag_recv,
):
    rows, cols = k_hbm.shape
    modes = u_hbm.shape[0]
    tiles = cols // 128
    columns = 4 * modes
    share = columns // ny
    px, py = lax.axis_index("gx"), lax.axis_index("gy")

    def fetch(i):
        return pltpu.make_async_copy(u_hbm.at[:, i, :], wide.at[i + 1], load.at[i])

    coefs = [
        pltpu.make_async_copy(k_hbm, kappa.at[pl.ds(8, rows)], load.at[rows]),
        pltpu.make_async_copy(p_hbm, p_ref, load.at[rows + 1]),
    ]

    def begin(i, _):
        fetch(i).start()
        return 0

    lax.fori_loop(0, rows, begin, 0)
    for copy in coefs:
        copy.start()
    barrier = pltpu.get_barrier_semaphore()
    for d in range(1, nx):
        pl.semaphore_signal(barrier, inc=1, device_id={"gx": lax.rem(px + d, nx)}, device_id_type=MESH)
    for d in range(1, ny):
        pl.semaphore_signal(barrier, inc=1, device_id={"gy": lax.rem(py + d, ny)}, device_id_type=MESH)

    lanes = lax.broadcasted_iota(jnp.int32, (modes, 128), 1)

    def collect(q, carry):
        first, last = carry
        for s in range(8):
            fetch(q * 8 + s).wait()
        for s in range(8):
            i = q * 8 + s
            first = jnp.where(lanes == i, pltpu.roll(wide[i + 1, :, :128], i, 1), first)
            last = jnp.where(lanes == i, pltpu.roll(wide[i + 1, :, cols - 128:], (i + 1) & 127, 1), last)
        return first, last

    zero = jnp.zeros((modes, 128), F32)
    first, last = lax.fori_loop(0, rows // 8, collect, (zero, zero))
    edge[0] = first
    edge[1] = last
    for copy in coefs:
        copy.wait()

    pl.semaphore_wait(barrier, nx + ny - 2)
    has_up, has_down, has_left, has_right = px > 0, px < nx - 1, py > 0, py < ny - 1
    down, up = {"gx": lax.rem(px + 1, nx)}, {"gx": lax.rem(px + nx - 1, nx)}
    right, left = {"gy": lax.rem(py + 1, ny)}, {"gy": lax.rem(py + ny - 1, ny)}
    own = pl.ds(8, rows)
    moves = (
        (wide.at[rows], wide.at[0], down, has_down, has_up),
        (kappa.at[pl.ds(rows, 8)], kappa.at[pl.ds(0, 8)], down, has_down, has_up),
        (wide.at[1], wide.at[rows + 1], up, has_up, has_down),
        (kappa.at[pl.ds(8, 8)], kappa.at[pl.ds(rows + 8, 8)], up, has_up, has_down),
        (edge.at[1], halo.at[0], right, has_right, has_left),
        (kappa.at[own, pl.ds(cols - 128, 128)], kside.at[0], right, has_right, has_left),
        (edge.at[0], halo.at[1], left, has_left, has_right),
        (kappa.at[own, pl.ds(0, 128)], kside.at[1], left, has_left, has_right),
    )
    copies = [
        (
            pltpu.make_async_remote_copy(
                src_ref=src, dst_ref=dst, send_sem=halo_send.at[n], recv_sem=halo_recv.at[n],
                device_id=device, device_id_type=MESH,
            ), sends, receives,
        )
        for n, (src, dst, device, sends, receives) in enumerate(moves)
    ]
    for n in range(0, len(copies), 2):
        @pl.when(copies[n][1])
        def _():
            copies[n][0].start()
            copies[n + 1][0].start()

    def put(block, i, value):
        high, low = split(value)
        at = pl.ds(pl.multiple_of(i * cols, cols), cols)
        m_ref[block * modes:(block + 1) * modes, at] = high
        m_ref[columns + block * modes:columns + (block + 1) * modes, at] = low

    def flux(i):
        return xface[pl.ds(i, 1), :] * (wide[i] - wide[i + 1])

    def inner(i, before):
        after = flux(i + 1)
        center = wide[i + 1]
        put(0, i, center)
        put(1, i, after - before)
        put(3, i, p_ref[pl.ds(i, 1), :] * center)
        return after

    xface[pl.ds(1, rows - 1), :] = 0.5 * (kappa[pl.ds(8, rows - 1), :] + kappa[pl.ds(9, rows - 1), :])

    def pair(g, before):
        return inner(2 * g + 2, inner(2 * g + 1, before))

    lax.fori_loop(0, (rows - 2) // 2, pair, flux(1))

    for copy, sends, receives in copies:
        @pl.when(sends)
        def _():
            copy.wait_send()

        @pl.when(receives)
        def _():
            copy.wait_recv()

    @pl.when(px == 0)
    def _():
        wide[0] = jnp.zeros((modes, cols), F32)
        kappa[pl.ds(0, 8), :] = jnp.zeros((8, cols), F32)

    @pl.when(px == nx - 1)
    def _():
        wide[rows + 1] = jnp.zeros((modes, cols), F32)
        kappa[pl.ds(rows + 8, 8), :] = jnp.zeros((8, cols), F32)

    @pl.when(py == 0)
    def _():
        halo[0] = zero
        kside[0] = jnp.zeros((rows, 128), F32)

    @pl.when(py == ny - 1)
    def _():
        halo[1] = zero
        kside[1] = jnp.zeros((rows, 128), F32)

    for i in (0, rows):
        xface[i:i + 1, :] = 0.5 * (kappa[i + 7:i + 8, :] + kappa[i + 8:i + 9, :])
    inner(0, flux(0))
    inner(rows - 1, flux(rows - 1))

    lane = lax.broadcasted_iota(jnp.int32, (rows, 128), 1)
    k_tile = [kappa[own, t * 128:(t + 1) * 128] for t in range(tiles)]
    turned = [pltpu.roll(k, 127, 1) for k in k_tile] + [pltpu.roll(kside[1], 127, 1)]
    for t in range(tiles):
        yface[:, t * 128:(t + 1) * 128] = 0.5 * (k_tile[t] + jnp.where(lane == 127, turned[t + 1], turned[t]))
    yleft[...] = 0.5 * (pltpu.roll(kside[0], 1, 1) + k_tile[0])

    group = 4
    acc[...] = jnp.zeros_like(acc)

    def product(g):
        at = pl.ds(pl.multiple_of(g * group * cols, group * cols), group * cols)
        acc[...] += lax.dot_general(
            m_ref[:columns, at], m_ref[:, at], (((1,), (1,)), ((), ())), preferred_element_type=F32
        )

    def build(g):
        for s in range(group):
            i = g * group + s
            u = [wide[i + 1, :, t * 128:(t + 1) * 128] for t in range(tiles)]
            r = [pltpu.roll(value, 127, 1) for value in u] + [pltpu.roll(halo[1], 127 - i, 1)]
            scale = yface[pl.ds(i, 1), :]
            f = [
                scale[:, t * 128:(t + 1) * 128] * (u[t] - jnp.where(lanes == 127, r[t + 1], r[t]))
                for t in range(tiles)
            ]
            outer = yleft[pl.ds(i, 1), :] * (pltpu.roll(halo[0], (128 - i) & 127, 1) - u[0])
            b = [outer] + [pltpu.roll(value, 1, 1) for value in f]
            along = [f[t] - jnp.where(lanes == 0, b[t], b[t + 1]) for t in range(tiles)]
            put(2, i, jnp.concatenate(along, 1))

    def advance(g, _):
        product(g - 1)
        build(g)
        return 0

    build(0)
    lax.fori_loop(1, rows // group, advance, 0)
    product(rows // group - 1)
    cross = acc[:, columns:]
    total = (acc[:, :columns] + (cross + cross.T)) * (1.0 / (rows * cols * nx * ny))
    for j in range(ny):
        part[j] = total[j * share:(j + 1) * share]

    copies = [
        pltpu.make_async_remote_copy(
            src_ref=part.at[lax.rem(py + d, ny)], dst_ref=piece.at[py], send_sem=rs_send.at[d], recv_sem=rs_recv.at[d],
            device_id={"gy": lax.rem(py + d, ny)}, device_id_type=MESH,
        )
        for d in range(1, ny)
    ]
    for copy in copies:
        copy.start()
    piece[py] = part[py]
    for copy in copies:
        copy.wait()
    ring[px] = functools.reduce(jnp.add, [piece[j] for j in range(ny)])

    copies = [
        pltpu.make_async_remote_copy(
            src_ref=ring.at[px], dst_ref=ring.at[px], send_sem=all_send.at[d], recv_sem=all_recv.at[d],
            device_id={"gx": lax.rem(px + d, nx)}, device_id_type=MESH,
        )
        for d in range(1, nx)
    ]
    for copy in copies:
        copy.start()
    for copy in copies:
        copy.wait()
    full[py] = functools.reduce(jnp.add, [ring[j] for j in range(nx)])

    copies = [
        pltpu.make_async_remote_copy(
            src_ref=full.at[py], dst_ref=full.at[py], send_sem=ag_send.at[d], recv_sem=ag_recv.at[d],
            device_id={"gy": lax.rem(py + d, ny)}, device_id_type=MESH,
        )
        for d in range(1, ny)
    ]
    for copy in copies:
        copy.start()
    for copy in copies:
        copy.wait()
    for j in range(ny):
        g_ref[j * share:(j + 1) * share, :] = full[j]


def gram(fields, conduct, potential, nx, ny):
    modes, rows, cols = fields.shape
    columns = 4 * modes
    vmem = pl.BlockSpec(memory_space=pltpu.VMEM)
    dma = pltpu.SemaphoreType.DMA
    return pl.pallas_call(
        functools.partial(gram_kernel, nx, ny),
        out_shape=(
            pltpu.VMEM((2 * columns, rows * cols), BF16),
            pltpu.VMEM((columns, columns), F32),
        ),
        in_specs=[pl.BlockSpec(memory_space=pltpu.HBM)] * 3,
        out_specs=(vmem, vmem),
        scratch_shapes=[
            pltpu.VMEM((rows + 2, modes, cols), F32),
            pltpu.VMEM((rows + 16, cols), F32),
            pltpu.VMEM((rows, cols), F32),
            pltpu.VMEM((rows + 8, cols), F32),
            pltpu.VMEM((rows, cols), F32),
            pltpu.VMEM((rows, 128), F32),
            pltpu.VMEM((2, modes, 128), F32),
            pltpu.VMEM((2, modes, 128), F32),
            pltpu.VMEM((2, rows, 128), F32),
            pltpu.VMEM((columns, 2 * columns), F32),
            pltpu.VMEM((ny, columns // ny, columns), F32),
            pltpu.VMEM((ny, columns // ny, columns), F32),
            pltpu.VMEM((nx, columns // ny, columns), F32),
            pltpu.VMEM((ny, columns // ny, columns), F32),
            dma((rows + 2,)),
            dma((8,)), dma((8,)), dma((ny,)), dma((ny,)), dma((nx,)), dma((nx,)), dma((ny,)), dma((ny,)),
        ],
        compiler_params=pltpu.CompilerParams(
            collective_id=0, has_side_effects=True, vmem_limit_bytes=28 * 1024 * 1024
        ),
        name="gram",
    )(*(pltpu.with_memory_space_constraint(a, pltpu.HBM) for a in (fields, conduct, potential)))


def factor(g_ref, r_ref, w_ref):
    size = g_ref.shape[0]
    block = 8
    panels = size // block
    lane = lax.broadcasted_iota(jnp.int32, (block, size), 1)
    sub = lax.broadcasted_iota(jnp.int32, (block, size), 0)

    def row(value, j):
        return jnp.broadcast_to(value[j:j + 1], (block, size))

    def column(value, j):
        return jnp.broadcast_to(value[:, j:j + 1], (block, size))

    z = [g_ref[i * block:(i + 1) * block, :] for i in range(panels)]
    for p in range(panels):
        at = p * block
        inside = (lane >= at) & (lane < at + block)
        cols = [column(z[p], at + j) for j in range(block)]
        plain = z[p]
        swept = jnp.where(inside, jnp.where(lane == at + sub, 1.0, 0.0), plain)
        solved = upper = jnp.zeros((block, size), F32)
        for j in range(block):
            root = lax.rsqrt(row(cols[j], j))
            low = cols[j] * root
            both = jnp.where(sub == j, -root, low)
            for k in range(j + 1, block):
                cols[k] = jnp.where(sub == j, 0.0, cols[k]) - both * row(low, k)
            line = row(swept, j) * root
            solved = jnp.where(sub == j, line, solved)
            swept = jnp.where(sub == j, 0.0, swept) - both * line
            line = row(plain, j) * root
            upper = jnp.where(sub == j, line, upper)
            plain = plain - low * line
        r_ref[at:at + block, :] = jnp.where(lane >= at + sub, upper, 0.0)
        w_ref[at:at + block, :] = jnp.where(lane <= at + sub, solved, 0.0)
        lines = [row(swept, k) for k in range(block)]
        heads = [[column(z[i], at + k) for i in range(p + 1, panels)] for k in range(block)]
        for i in range(p + 1, panels):
            terms = [heads[k][i - p - 1] * lines[k] for k in range(block)]
            z[i] = jnp.where(inside, 0.0, z[i]) - functools.reduce(jnp.add, terms)


def apply_kernel(g_ref, m_ref, o_hbm, r_ref, w_ref, weights, out, sent):
    rows, columns, cols = out.shape
    factor(g_ref, r_ref, w_ref)
    high, low = split(w_ref[...])
    weights[:columns, :columns] = high
    weights[:columns, columns:] = high
    weights[columns:, :columns] = low
    weights[columns:, columns:] = jnp.zeros_like(low)
    group = 16

    def send(i):
        return pltpu.make_async_copy(out.at[i], o_hbm.at[:, i, :], sent.at[i])

    def step(g, _):
        for s in range(group):
            i = g * group + s
            at = pl.ds(pl.multiple_of(i * cols, cols), cols)
            both = jnp.dot(weights[...], m_ref[:, at], preferred_element_type=F32)
            out[i] = both[:columns] + both[columns:]
        for s in range(group):
            send(g * group + s).start()
        return 0

    def finish(i, _):
        send(i).wait()
        return 0

    lax.fori_loop(0, rows // group, step, 0)
    lax.fori_loop(0, rows, finish, 0)


def apply(total, matrix, rows, cols):
    columns = total.shape[0]
    vmem = pl.BlockSpec(memory_space=pltpu.VMEM)
    return pl.pallas_call(
        apply_kernel,
        out_shape=(
            jax.ShapeDtypeStruct((columns, rows, cols), F32),
            jax.ShapeDtypeStruct((columns, columns), F32),
        ),
        in_specs=[vmem, vmem],
        out_specs=(pl.BlockSpec(memory_space=pltpu.HBM), vmem),
        scratch_shapes=[
            pltpu.VMEM((columns, columns), F32),
            pltpu.VMEM((2 * columns, 2 * columns), BF16),
            pltpu.VMEM((rows, columns, cols), F32),
            pltpu.SemaphoreType.DMA((rows,)),
        ],
        compiler_params=pltpu.CompilerParams(vmem_limit_bytes=20 * 1024 * 1024),
        name="apply",
    )(total, pltpu.with_memory_space_constraint(matrix, pltpu.VMEM))


def on_device(nx, ny, mode_fields, conductance, potential):
    _, rows, cols = mode_fields.shape
    matrix, total = gram(mode_fields, conductance, potential, nx, ny)
    return apply(total, matrix, rows, cols)


def solution(mesh):
    placed = (P(None, "gx", "gy"), P("gx", "gy"), P("gx", "gy"))
    return jax.shard_map(
        functools.partial(on_device, mesh.shape["gx"], mesh.shape["gy"]),
        mesh=mesh, in_specs=placed, out_specs=(P(None, "gx", "gy"), P()), check_vma=False,
    )
```

```python
import functools

import jax
import jax.numpy as jnp
from jax import lax
from jax.experimental import pallas as pl
from jax.experimental.pallas import tpu as pltpu
from jax.sharding import PartitionSpec as P

MESH = pl.DeviceIdType.MESH
F32 = jnp.float32
BF16 = jnp.bfloat16


def split(value):
    high = value.astype(BF16)
    return high, (value - high.astype(F32)).astype(BF16)


def gram_kernel(
    nx, ny, u_hbm, k_hbm, p_hbm, m_ref, g_ref,
    wide, kappa, p_ref, xface, yface, edge, halo, inside, acc, part, piece, ring, full,
    load, halo_send, halo_recv, rs_send, rs_recv, all_send, all_recv, ag_send, ag_recv,
):
    rows, cols = k_hbm.shape
    modes = u_hbm.shape[0]
    tiles = cols // 128
    columns = 4 * modes
    share = columns // ny
    px, py = lax.axis_index("gx"), lax.axis_index("gy")

    def fetch(i):
        return pltpu.make_async_copy(u_hbm.at[:, i, :], wide.at[i + 1], load.at[i])

    own = pl.ds(8, rows)
    load_k = pltpu.make_async_copy(k_hbm, kappa.at[own], load.at[rows])
    load_p = pltpu.make_async_copy(p_hbm, p_ref, load.at[rows + 1])

    def begin(i, _):
        fetch(i).start()
        return 0

    load_k.start()
    lax.fori_loop(0, rows, begin, 0)
    load_p.start()
    barrier = pltpu.get_barrier_semaphore()
    for d in range(1, nx):
        pl.semaphore_signal(barrier, inc=1, device_id={"gx": lax.rem(px + d, nx)}, device_id_type=MESH)
    for d in range(1, ny):
        pl.semaphore_signal(barrier, inc=1, device_id={"gy": lax.rem(py + d, ny)}, device_id_type=MESH)

    def iota(height):
        return lax.broadcasted_iota(jnp.int32, (height, 128), 1)

    lanes = iota(modes)
    packed = iota(modes + 8)
    holder = ((packed + 1) & 127) >> 1
    load_k.wait()

    def collect(q, pack):
        for s in range(8):
            fetch(q * 8 + s).wait()
        for s in range(8):
            i = q * 8 + s
            k_row = jnp.broadcast_to(kappa[pl.ds(i + 8, 1), :], (8, cols))
            first = jnp.concatenate([wide[i + 1, :, :128], k_row[:, :128]], 0)
            last = jnp.concatenate([wide[i + 1, :, cols - 128:], k_row[:, cols - 128:]], 0)
            pack = jnp.where(holder == i, pltpu.roll(jnp.where(packed == 0, first, last), 2 * i, 1), pack)
        return pack

    edge[...] = lax.fori_loop(0, rows // 8, collect, jnp.zeros((modes + 8, 128), F32))

    pl.semaphore_wait(barrier, nx + ny - 2)
    has_up, has_down, has_left, has_right = px > 0, px < nx - 1, py > 0, py < ny - 1
    down, up = {"gx": lax.rem(px + 1, nx)}, {"gx": lax.rem(px + nx - 1, nx)}
    right, left = {"gy": lax.rem(py + 1, ny)}, {"gy": lax.rem(py + ny - 1, ny)}
    moves = (
        (wide.at[rows], wide.at[0], down, has_down, has_up),
        (kappa.at[pl.ds(rows, 8)], kappa.at[pl.ds(0, 8)], down, has_down, has_up),
        (wide.at[1], wide.at[rows + 1], up, has_up, has_down),
        (kappa.at[pl.ds(8, 8)], kappa.at[pl.ds(rows + 8, 8)], up, has_up, has_down),
        (edge, halo.at[0], right, has_right, has_left),
        (edge, halo.at[1], left, has_left, has_right),
    )
    copies = [
        (
            pltpu.make_async_remote_copy(
                src_ref=src, dst_ref=dst, send_sem=halo_send.at[n], recv_sem=halo_recv.at[n],
                device_id=device, device_id_type=MESH,
            ), sends, receives,
        )
        for n, (src, dst, device, sends, receives) in enumerate(moves)
    ]
    for copy, sends, _ in copies:
        @pl.when(sends)
        def _():
            copy.start()

    def put(block, i, value):
        high, low = split(value)
        at = pl.ds(pl.multiple_of(i * cols, cols), cols)
        m_ref[block * modes:(block + 1) * modes, at] = high
        m_ref[columns + block * modes:columns + (block + 1) * modes, at] = low

    def flux(i):
        return xface[pl.ds(i, 1), :] * (wide[i] - wide[i + 1])

    xface[pl.ds(1, rows - 1), :] = 0.5 * (kappa[pl.ds(8, rows - 1), :] + kappa[pl.ds(9, rows - 1), :])
    lane = iota(rows)
    k_tile = [kappa[own, t * 128:(t + 1) * 128] for t in range(tiles)]
    turned = [pltpu.roll(k, 127, 1) for k in k_tile]
    for t in range(tiles):
        face = 0.5 * (k_tile[t] + (jnp.where(lane == 127, turned[t + 1], turned[t]) if t + 1 < tiles else turned[t]))
        yface[:, t * 128:(t + 1) * 128] = face if t + 1 < tiles else jnp.where(lane == 127, 0.0, face)
    load_p.wait()

    def local(i):
        center = wide[i + 1]
        put(0, i, center)
        put(3, i, p_ref[pl.ds(i, 1), :] * center)
        u = [center[:, t * 128:(t + 1) * 128] for t in range(tiles)]
        r = [pltpu.roll(value, 127, 1) for value in u]
        scale = yface[pl.ds(i, 1), :]
        f = [
            scale[:, t * 128:(t + 1) * 128] * (u[t] - (jnp.where(lanes == 127, r[t + 1], r[t]) if t + 1 < tiles else r[t]))
            for t in range(tiles)
        ]
        b = [pltpu.roll(value, 1, 1) for value in f]
        for t in range(tiles):
            inside[i, :, t * 128:(t + 1) * 128] = f[t] - jnp.where(lanes == 0, b[t - 1], b[t])

    group = 16

    def inner(first, count, before):
        for s in range(group):
            local(first + s)
            if s < count:
                after = flux(first + s + 2)
                put(1, first + s + 1, after - before)
                before = after
        return before

    def sweep(g, before):
        return inner(g * group, group, before)

    inner(rows - group, group - 2, lax.fori_loop(0, rows // group - 1, sweep, flux(1)))

    for copy, sends, receives in copies:
        @pl.when(sends)
        def _():
            copy.wait_send()

        @pl.when(receives)
        def _():
            copy.wait_recv()

    @pl.when(px == 0)
    def _():
        wide[0] = jnp.zeros((modes, cols), F32)
        kappa[pl.ds(0, 8), :] = jnp.zeros((8, cols), F32)

    @pl.when(px == nx - 1)
    def _():
        wide[rows + 1] = jnp.zeros((modes, cols), F32)
        kappa[pl.ds(rows + 8, 8), :] = jnp.zeros((8, cols), F32)

    @pl.when(py == 0)
    def _():
        halo[0] = jnp.zeros((modes + 8, 128), F32)

    @pl.when(py == ny - 1)
    def _():
        halo[1] = jnp.zeros((modes + 8, 128), F32)

    for i in (0, rows):
        xface[i:i + 1, :] = 0.5 * (kappa[i + 7:i + 8, :] + kappa[i + 8:i + 9, :])
    for i in (0, rows - 1):
        put(1, i, flux(i + 1) - flux(i))
    mine = edge[...]
    other = jnp.where((packed & 1) == 0, pltpu.roll(halo[0], 1, 1), pltpu.roll(halo[1], 127, 1))
    across = 0.5 * (mine[modes:modes + 1] + other[modes:modes + 1]) * (mine[:modes] - other[:modes])

    acc[...] = jnp.zeros_like(acc)

    def build(g, _):
        for s in range(group):
            i = g * group + s
            turn = pltpu.roll(across, (128 - 2 * i) & 127, 1)
            y = [inside[i, :, t * 128:(t + 1) * 128] for t in range(tiles)]
            y[0] = y[0] + jnp.where(lanes == 0, turn, 0.0)
            y[-1] = y[-1] + jnp.where(lanes == 127, turn, 0.0)
            put(2, i, jnp.concatenate(y, 1))
        at = pl.ds(pl.multiple_of(g * group * cols, group * cols), group * cols)
        acc[...] += lax.dot_general(
            m_ref[:, at], m_ref[:columns, at], (((1,), (1,)), ((), ())), preferred_element_type=F32
        )
        return 0

    lax.fori_loop(0, rows // group, build, 0)
    cross = acc[columns:]
    total = (acc[:columns] + (cross + cross.T)) * (1.0 / (rows * cols * nx * ny))
    for j in range(ny):
        part[j] = total[j * share:(j + 1) * share]

    copies = [
        pltpu.make_async_remote_copy(
            src_ref=part.at[lax.rem(py + d, ny)], dst_ref=piece.at[py], send_sem=rs_send.at[d], recv_sem=rs_recv.at[d],
            device_id={"gy": lax.rem(py + d, ny)}, device_id_type=MESH,
        )
        for d in range(1, ny)
    ]
    for copy in copies:
        copy.start()
    piece[py] = part[py]
    for copy in copies:
        copy.wait()
    ring[px] = functools.reduce(jnp.add, [piece[j] for j in range(ny)])

    copies = [
        pltpu.make_async_remote_copy(
            src_ref=ring.at[px], dst_ref=ring.at[px], send_sem=all_send.at[d], recv_sem=all_recv.at[d],
            device_id={"gx": lax.rem(px + d, nx)}, device_id_type=MESH,
        )
        for d in range(1, nx)
    ]
    for copy in copies:
        copy.start()
    for copy in copies:
        copy.wait()
    full[py] = functools.reduce(jnp.add, [ring[j] for j in range(nx)])

    copies = [
        pltpu.make_async_remote_copy(
            src_ref=full.at[py], dst_ref=full.at[py], send_sem=ag_send.at[d], recv_sem=ag_recv.at[d],
            device_id={"gy": lax.rem(py + d, ny)}, device_id_type=MESH,
        )
        for d in range(1, ny)
    ]
    for copy in copies:
        copy.start()
    for copy in copies:
        copy.wait()
    for j in range(ny):
        g_ref[j * share:(j + 1) * share, :] = full[j]


def gram(fields, conduct, potential, nx, ny):
    modes, rows, cols = fields.shape
    columns = 4 * modes
    vmem = pl.BlockSpec(memory_space=pltpu.VMEM)
    dma = pltpu.SemaphoreType.DMA
    return pl.pallas_call(
        functools.partial(gram_kernel, nx, ny),
        out_shape=(
            pltpu.VMEM((2 * columns, rows * cols), BF16),
            pltpu.VMEM((columns, columns), F32),
        ),
        in_specs=[pl.BlockSpec(memory_space=pltpu.HBM)] * 3,
        out_specs=(vmem, vmem),
        scratch_shapes=[
            pltpu.VMEM((rows + 2, modes, cols), F32),
            pltpu.VMEM((rows + 16, cols), F32),
            pltpu.VMEM((rows, cols), F32),
            pltpu.VMEM((rows + 8, cols), F32),
            pltpu.VMEM((rows, cols), F32),
            pltpu.VMEM((modes + 8, 128), F32),
            pltpu.VMEM((2, modes + 8, 128), F32),
            pltpu.VMEM((rows, modes, cols), F32),
            pltpu.VMEM((2 * columns, columns), F32),
            pltpu.VMEM((ny, columns // ny, columns), F32),
            pltpu.VMEM((ny, columns // ny, columns), F32),
            pltpu.VMEM((nx, columns // ny, columns), F32),
            pltpu.VMEM((ny, columns // ny, columns), F32),
            dma((rows + 2,)),
            dma((6,)), dma((6,)), dma((ny,)), dma((ny,)), dma((nx,)), dma((nx,)), dma((ny,)), dma((ny,)),
        ],
        compiler_params=pltpu.CompilerParams(
            collective_id=0, has_side_effects=True, vmem_limit_bytes=28 * 1024 * 1024
        ),
        name="gram",
    )(*(pltpu.with_memory_space_constraint(a, pltpu.HBM) for a in (fields, conduct, potential)))


def factor(g_ref, r_ref, w_ref):
    size = g_ref.shape[0]
    block, width = 8, 16
    parts, tiles = width // block, size // block
    lane = lax.broadcasted_iota(jnp.int32, (block, size), 1)
    sub = lax.broadcasted_iota(jnp.int32, (block, size), 0)

    def row(value, j):
        return jnp.broadcast_to(value[j:j + 1], (block, size))

    def column(value, j):
        return jnp.broadcast_to(value[:, j:j + 1], (block, size))

    z = [g_ref[i * block:(i + 1) * block, :] for i in range(tiles)]
    for at in range(0, size, width):
        if at == size // 2:
            yield
        start = at // block
        stop = start + parts
        inside = (lane >= at) & (lane < at + width)
        cols = [[column(value, at + k) for value in z[start:stop]] for k in range(width)]
        plain = z[start:stop]
        swept = [
            jnp.where(inside, jnp.where(lane == at + h * block + sub, 1.0, 0.0), value)
            for h, value in enumerate(plain)
        ]
        solved = [jnp.zeros((block, size), F32)] * parts
        upper = list(solved)
        for j in range(width):
            h, s = divmod(j, block)
            root = lax.rsqrt(row(cols[j][h], s))
            low = [value * root for value in cols[j]]
            both = list(low)
            both[h] = jnp.where(sub == s, -root, low[h])

            def sweep(values, line):
                return [
                    (jnp.where(sub == s, 0.0, value) if q == h else value) - both[q] * line
                    for q, value in enumerate(values)
                ]

            for k in range(j + 1, width):
                cols[k] = sweep(cols[k], row(low[k // block], k % block))
            line = row(swept[h], s) * root
            solved[h] = jnp.where(sub == s, line, solved[h])
            swept = sweep(swept, line)
            line = row(plain[h], s) * root
            upper[h] = jnp.where(sub == s, line, upper[h])
            plain = [value if q < h else value - low[q] * line for q, value in enumerate(plain)]
        for h in range(parts):
            first = at + h * block
            r_ref[first:first + block, :] = jnp.where(lane >= first + sub, upper[h], 0.0)
            w_ref[first:first + block, :] = jnp.where(lane <= first + sub, solved[h], 0.0)
        for i in range(stop, min(stop + parts, tiles)):
            terms = [column(z[i], at + k) * row(swept[k // block], k % block) for k in range(width)]
            while len(terms) > 1:
                terms = [x + y for x, y in zip(terms[::2], terms[1::2])]
            z[i] = jnp.where(inside, 0.0, z[i]) - terms[0]
        if stop + parts < tiles:
            pads = [jnp.zeros((at, size), F32)] * (at > 0)
            sides = jnp.concatenate(pads + swept + [jnp.zeros((size - at - width, size), F32)], 0)
            change = jnp.dot(
                jnp.concatenate(z[stop + parts:], 0), sides,
                preferred_element_type=F32, precision=lax.Precision.HIGHEST,
            )
            for n, i in enumerate(range(stop + parts, tiles)):
                z[i] = jnp.where(inside, 0.0, z[i]) - change[n * block:(n + 1) * block]
    yield


def apply_kernel(g_ref, m_ref, o_hbm, r_ref, w_ref, upper, lower, out, sent):
    rows, columns, cols = out.shape
    half = columns // 2
    group = 16
    steps = factor(g_ref, r_ref, w_ref)

    def send(side, i):
        part = pl.ds(side * half, half)
        return pltpu.make_async_copy(out.at[i, part], o_hbm.at[part, i, :], sent)

    def over(side, value):
        def step(g, _):
            for s in range(group):
                i = g * group + s
                out[i, side * half:(side + 1) * half, :] = value(pl.ds(pl.multiple_of(i * cols, cols), cols))
            for s in range(group):
                send(side, g * group + s).start()
            return 0

        lax.fori_loop(0, rows // group, step, 0)

    next(steps)
    high, low = split(w_ref[:half, :])
    upper[...] = jnp.concatenate([high[:, :half], high[:, :half], low[:, :half]], 1)

    def first(at):
        near = m_ref[:half, at]
        right = jnp.concatenate([near, m_ref[columns:columns + half, at], near], 0)
        return jnp.dot(upper[...], right, preferred_element_type=F32)

    over(0, first)
    next(steps)
    high, low = split(w_ref[half:, :])
    lower[:half, :columns] = high
    lower[:half, columns:] = high
    lower[half:, :columns] = low
    lower[half:, columns:] = jnp.zeros_like(low)

    def second(at):
        both = jnp.dot(lower[...], m_ref[:, at], preferred_element_type=F32)
        return both[:half] + both[half:]

    over(1, second)

    pltpu.make_async_copy(out, out, sent).wait()


def apply(total, matrix, rows, cols):
    columns = total.shape[0]
    vmem = pl.BlockSpec(memory_space=pltpu.VMEM)
    return pl.pallas_call(
        apply_kernel,
        out_shape=(
            jax.ShapeDtypeStruct((columns, rows, cols), F32),
            jax.ShapeDtypeStruct((columns, columns), F32),
        ),
        in_specs=[vmem, vmem],
        out_specs=(pl.BlockSpec(memory_space=pltpu.HBM), vmem),
        scratch_shapes=[
            pltpu.VMEM((columns, columns), F32),
            pltpu.VMEM((columns // 2, 3 * columns // 2), BF16),
            pltpu.VMEM((columns, 2 * columns), BF16),
            pltpu.VMEM((rows, columns, cols), F32),
            pltpu.SemaphoreType.DMA,
        ],
        compiler_params=pltpu.CompilerParams(vmem_limit_bytes=20 * 1024 * 1024),
        name="apply",
    )(total, pltpu.with_memory_space_constraint(matrix, pltpu.VMEM))


def on_device(nx, ny, mode_fields, conductance, potential):
    _, rows, cols = mode_fields.shape
    matrix, total = gram(mode_fields, conductance, potential, nx, ny)
    return apply(total, matrix, rows, cols)


def solution(mesh):
    placed = (P(None, "gx", "gy"), P("gx", "gy"), P("gx", "gy"))
    return jax.shard_map(
        functools.partial(on_device, mesh.shape["gx"], mesh.shape["gy"]),
        mesh=mesh, in_specs=placed, out_specs=(P(None, "gx", "gy"), P()), check_vma=False,
    )
```

```python
import functools

import jax
import jax.numpy as jnp
from jax import lax
from jax.experimental import pallas as pl
from jax.experimental.pallas import tpu as pltpu
from jax.sharding import PartitionSpec as P

MESH = pl.DeviceIdType.MESH
F32 = jnp.float32
BF16 = jnp.bfloat16


def split(value):
    high = value.astype(BF16)
    return high, (value - high.astype(F32)).astype(BF16)


def gram_kernel(
    nx, ny, u_hbm, k_hbm, p_hbm, m_ref, g_ref,
    wide, kappa, p_ref, xface, yface, edge, halo, turned, flow, back, acc, part, piece, ring, full,
    load, halo_send, halo_recv, rs_send, rs_recv, all_send, all_recv, ag_send, ag_recv,
):
    rows, cols = k_hbm.shape
    modes = u_hbm.shape[0]
    tiles = cols // 128
    columns = 4 * modes
    share = columns // ny
    px, py = lax.axis_index("gx"), lax.axis_index("gy")

    def fetch(i):
        return pltpu.make_async_copy(u_hbm.at[:, i, :], wide.at[i + 1], load.at[i])

    own = pl.ds(8, rows)
    load_k = pltpu.make_async_copy(k_hbm, kappa.at[own], load.at[rows])
    load_p = pltpu.make_async_copy(p_hbm, p_ref, load.at[rows + 1])

    def begin(i, _):
        fetch(i).start()
        return 0

    load_k.start()
    lax.fori_loop(0, rows, begin, 0)
    load_p.start()
    barrier = pltpu.get_barrier_semaphore()
    for d in range(1, nx):
        pl.semaphore_signal(barrier, inc=1, device_id={"gx": lax.rem(px + d, nx)}, device_id_type=MESH)
    for d in range(1, ny):
        pl.semaphore_signal(barrier, inc=1, device_id={"gy": lax.rem(py + d, ny)}, device_id_type=MESH)

    def iota(height):
        return lax.broadcasted_iota(jnp.int32, (height, 128), 1)

    lanes = iota(modes)
    packed = iota(modes + 8)
    holder = ((packed + 1) & 127) >> 1
    load_k.wait()

    def collect(q, pack):
        for s in range(8):
            fetch(q * 8 + s).wait()
        for s in range(8):
            i = q * 8 + s
            k_row = jnp.broadcast_to(kappa[pl.ds(i + 8, 1), :], (8, cols))
            first = jnp.concatenate([wide[i + 1, :, :128], k_row[:, :128]], 0)
            last = jnp.concatenate([wide[i + 1, :, cols - 128:], k_row[:, cols - 128:]], 0)
            pack = jnp.where(holder == i, pltpu.roll(jnp.where(packed == 0, first, last), 2 * i, 1), pack)
        return pack

    edge[...] = lax.fori_loop(0, rows // 8, collect, jnp.zeros((modes + 8, 128), F32))

    pl.semaphore_wait(barrier, nx + ny - 2)
    has_up, has_down, has_left, has_right = px > 0, px < nx - 1, py > 0, py < ny - 1
    down, up = {"gx": lax.rem(px + 1, nx)}, {"gx": lax.rem(px + nx - 1, nx)}
    right, left = {"gy": lax.rem(py + 1, ny)}, {"gy": lax.rem(py + ny - 1, ny)}
    moves = (
        (wide.at[rows], wide.at[0], down, has_down, has_up),
        (kappa.at[pl.ds(rows, 8)], kappa.at[pl.ds(0, 8)], down, has_down, has_up),
        (wide.at[1], wide.at[rows + 1], up, has_up, has_down),
        (kappa.at[pl.ds(8, 8)], kappa.at[pl.ds(rows + 8, 8)], up, has_up, has_down),
        (edge, halo.at[0], right, has_right, has_left),
        (edge, halo.at[1], left, has_left, has_right),
    )
    copies = [
        (
            pltpu.make_async_remote_copy(
                src_ref=src, dst_ref=dst, send_sem=halo_send.at[n], recv_sem=halo_recv.at[n],
                device_id=device, device_id_type=MESH,
            ), sends, receives,
        )
        for n, (src, dst, device, sends, receives) in enumerate(moves)
    ]
    for copy, sends, _ in copies:
        @pl.when(sends)
        def _():
            copy.start()

    def put(block, i, value):
        high, low = split(value)
        at = pl.ds(pl.multiple_of(i * cols, cols), cols)
        m_ref[block * modes:(block + 1) * modes, at] = high
        m_ref[columns + block * modes:columns + (block + 1) * modes, at] = low

    def flux(i):
        return xface[pl.ds(i, 1), :] * (wide[i] - wide[i + 1])

    xface[pl.ds(1, rows - 1), :] = 0.5 * (kappa[pl.ds(8, rows - 1), :] + kappa[pl.ds(9, rows - 1), :])
    lane = iota(rows)

    def tile(t):
        return slice(t * 128, (t + 1) * 128)

    k_tile = [kappa[own, t * 128:(t + 1) * 128] for t in range(tiles)]
    k_next = [pltpu.roll(k, 127, 1) for k in k_tile]
    for t in range(tiles):
        face = 0.5 * (k_tile[t] + (jnp.where(lane == 127, k_next[t + 1], k_next[t]) if t + 1 < tiles else k_next[t]))
        yface[:, t * 128:(t + 1) * 128] = face if t + 1 < tiles else jnp.where(lane == 127, 0.0, face)
    load_p.wait()

    def local(i):
        center = wide[i + 1]
        put(0, i, center)
        put(3, i, p_ref[pl.ds(i, 1), :] * center)
        for t in range(tiles):
            turned[i, :, tile(t)] = pltpu.roll(center[:, tile(t)], 127, 1)

    def stream(g, _):
        for s in range(group):
            i = g * group + s
            scale = yface[pl.ds(i, 1), :]
            r = [turned[i, :, tile(t)] for t in range(tiles)]
            for t in range(tiles):
                after = jnp.where(lanes == 127, r[t + 1], r[t]) if t + 1 < tiles else r[t]
                f = scale[:, tile(t)] * (wide[i + 1, :, tile(t)] - after)
                flow[i, :, tile(t)] = f
                back[i, :, tile(t)] = pltpu.roll(f, 1, 1)
        return 0

    group = 16

    def inner(first, count, before):
        for s in range(group):
            local(first + s)
            if s < count:
                after = flux(first + s + 2)
                put(1, first + s + 1, after - before)
                before = after
        return before

    def sweep(g, before):
        return inner(g * group, group, before)

    inner(rows - group, group - 2, lax.fori_loop(0, rows // group - 1, sweep, flux(1)))
    lax.fori_loop(0, rows // group, stream, 0)

    for copy, sends, receives in copies:
        @pl.when(sends)
        def _():
            copy.wait_send()

        @pl.when(receives)
        def _():
            copy.wait_recv()

    @pl.when(px == 0)
    def _():
        wide[0] = jnp.zeros((modes, cols), F32)
        kappa[pl.ds(0, 8), :] = jnp.zeros((8, cols), F32)

    @pl.when(px == nx - 1)
    def _():
        wide[rows + 1] = jnp.zeros((modes, cols), F32)
        kappa[pl.ds(rows + 8, 8), :] = jnp.zeros((8, cols), F32)

    @pl.when(py == 0)
    def _():
        halo[0] = jnp.zeros((modes + 8, 128), F32)

    @pl.when(py == ny - 1)
    def _():
        halo[1] = jnp.zeros((modes + 8, 128), F32)

    for i in (0, rows):
        xface[i:i + 1, :] = 0.5 * (kappa[i + 7:i + 8, :] + kappa[i + 8:i + 9, :])
    for i in (0, rows - 1):
        put(1, i, flux(i + 1) - flux(i))
    mine = edge[...]
    other = jnp.where((packed & 1) == 0, pltpu.roll(halo[0], 1, 1), pltpu.roll(halo[1], 127, 1))
    across = 0.5 * (mine[modes:modes + 1] + other[modes:modes + 1]) * (mine[:modes] - other[:modes])

    acc[...] = jnp.zeros_like(acc)

    def build(g, _):
        for s in range(32):
            i = g * 32 + s
            turn = pltpu.roll(across, (128 - 2 * i) & 127, 1)
            b = [back[i, :, tile(t)] for t in range(tiles)]
            y = [flow[i, :, tile(t)] - jnp.where(lanes == 0, b[t - 1], b[t]) for t in range(tiles)]
            y[0] = y[0] + jnp.where(lanes == 0, turn, 0.0)
            y[-1] = y[-1] + jnp.where(lanes == 127, turn, 0.0)
            put(2, i, jnp.concatenate(y, 1))
        at = pl.ds(pl.multiple_of(g * 32 * cols, 32 * cols), 32 * cols)
        acc[...] += lax.dot_general(
            m_ref[:, at], m_ref[:columns, at], (((1,), (1,)), ((), ())), preferred_element_type=F32
        )
        return 0

    lax.fori_loop(0, rows // 32, build, 0)
    cross = acc[columns:]
    total = (acc[:columns] + (cross + cross.T)) * (1.0 / (rows * cols * nx * ny))
    for j in range(ny):
        part[j] = total[j * share:(j + 1) * share]

    copies = [
        pltpu.make_async_remote_copy(
            src_ref=part.at[lax.rem(py + d, ny)], dst_ref=piece.at[py], send_sem=rs_send.at[d], recv_sem=rs_recv.at[d],
            device_id={"gy": lax.rem(py + d, ny)}, device_id_type=MESH,
        )
        for d in range(1, ny)
    ]
    for copy in copies:
        copy.start()
    piece[py] = part[py]
    for copy in copies:
        copy.wait()
    ring[px] = functools.reduce(jnp.add, [piece[j] for j in range(ny)])

    copies = [
        pltpu.make_async_remote_copy(
            src_ref=ring.at[px], dst_ref=ring.at[px], send_sem=all_send.at[d], recv_sem=all_recv.at[d],
            device_id={"gx": lax.rem(px + d, nx)}, device_id_type=MESH,
        )
        for d in range(1, nx)
    ]
    for copy in copies:
        copy.start()
    for copy in copies:
        copy.wait()
    full[py] = functools.reduce(jnp.add, [ring[j] for j in range(nx)])

    copies = [
        pltpu.make_async_remote_copy(
            src_ref=full.at[py], dst_ref=full.at[py], send_sem=ag_send.at[d], recv_sem=ag_recv.at[d],
            device_id={"gy": lax.rem(py + d, ny)}, device_id_type=MESH,
        )
        for d in range(1, ny)
    ]
    for copy in copies:
        copy.start()
    for copy in copies:
        copy.wait()
    for j in range(ny):
        g_ref[j * share:(j + 1) * share, :] = full[j]


def gram(fields, conduct, potential, nx, ny):
    modes, rows, cols = fields.shape
    columns = 4 * modes
    vmem = pl.BlockSpec(memory_space=pltpu.VMEM)
    dma = pltpu.SemaphoreType.DMA
    return pl.pallas_call(
        functools.partial(gram_kernel, nx, ny),
        out_shape=(
            pltpu.VMEM((2 * columns, rows * cols), BF16),
            pltpu.VMEM((columns, columns), F32),
        ),
        in_specs=[pl.BlockSpec(memory_space=pltpu.HBM)] * 3,
        out_specs=(vmem, vmem),
        scratch_shapes=[
            pltpu.VMEM((rows + 2, modes, cols), F32),
            pltpu.VMEM((rows + 16, cols), F32),
            pltpu.VMEM((rows, cols), F32),
            pltpu.VMEM((rows + 8, cols), F32),
            pltpu.VMEM((rows, cols), F32),
            pltpu.VMEM((modes + 8, 128), F32),
            pltpu.VMEM((2, modes + 8, 128), F32),
            pltpu.VMEM((rows, modes, cols), F32),
            pltpu.VMEM((rows, modes, cols), F32),
            pltpu.VMEM((rows, modes, cols), F32),
            pltpu.VMEM((2 * columns, columns), F32),
            pltpu.VMEM((ny, columns // ny, columns), F32),
            pltpu.VMEM((ny, columns // ny, columns), F32),
            pltpu.VMEM((nx, columns // ny, columns), F32),
            pltpu.VMEM((ny, columns // ny, columns), F32),
            dma((rows + 2,)),
            dma((6,)), dma((6,)), dma((ny,)), dma((ny,)), dma((nx,)), dma((nx,)), dma((ny,)), dma((ny,)),
        ],
        compiler_params=pltpu.CompilerParams(
            collective_id=0, has_side_effects=True, vmem_limit_bytes=28 * 1024 * 1024
        ),
        name="gram",
    )(*(pltpu.with_memory_space_constraint(a, pltpu.HBM) for a in (fields, conduct, potential)))


def factor(g_ref, r_ref, w_ref):
    size = g_ref.shape[0]
    block, width = 8, 16
    parts, tiles = width // block, size // block
    lane = lax.broadcasted_iota(jnp.int32, (block, size), 1)
    sub = lax.broadcasted_iota(jnp.int32, (block, size), 0)

    def row(value, j):
        return jnp.broadcast_to(value[j:j + 1], (block, size))

    def column(value, j):
        return jnp.broadcast_to(value[:, j:j + 1], (block, size))

    z = [g_ref[i * block:(i + 1) * block, :] for i in range(tiles)]
    for at in range(0, size, width):
        if at == size // 2:
            yield
        start = at // block
        stop = start + parts
        inside = (lane >= at) & (lane < at + width)
        cols = [[column(value, at + k) for value in z[start:stop]] for k in range(width)]
        plain = z[start:stop]
        swept = [
            jnp.where(inside, jnp.where(lane == at + h * block + sub, 1.0, 0.0), value)
            for h, value in enumerate(plain)
        ]
        solved = [jnp.zeros((block, size), F32)] * parts
        upper = list(solved)
        for j in range(width):
            h, s = divmod(j, block)
            root = lax.rsqrt(row(cols[j][h], s))
            low = [value * root for value in cols[j]]
            both = list(low)
            both[h] = jnp.where(sub == s, -root, low[h])

            def sweep(values, line):
                return [
                    (jnp.where(sub == s, 0.0, value) if q == h else value) - both[q] * line
                    for q, value in enumerate(values)
                ]

            for k in range(j + 1, width):
                cols[k] = sweep(cols[k], row(low[k // block], k % block))
            line = row(swept[h], s) * root
            solved[h] = jnp.where(sub == s, line, solved[h])
            swept = sweep(swept, line)
            line = row(plain[h], s) * root
            upper[h] = jnp.where(sub == s, line, upper[h])
            plain = [value if q < h else value - low[q] * line for q, value in enumerate(plain)]
        for h in range(parts):
            first = at + h * block
            r_ref[first:first + block, :] = jnp.where(lane >= first + sub, upper[h], 0.0)
            w_ref[first:first + block, :] = jnp.where(lane <= first + sub, solved[h], 0.0)
        for i in range(stop, min(stop + parts, tiles)):
            terms = [column(z[i], at + k) * row(swept[k // block], k % block) for k in range(width)]
            while len(terms) > 1:
                terms = [x + y for x, y in zip(terms[::2], terms[1::2])]
            z[i] = jnp.where(inside, 0.0, z[i]) - terms[0]
        if stop + parts < tiles:
            pads = [jnp.zeros((at, size), F32)] * (at > 0)
            sides = jnp.concatenate(pads + swept + [jnp.zeros((size - at - width, size), F32)], 0)
            change = jnp.dot(
                jnp.concatenate(z[stop + parts:], 0), sides,
                preferred_element_type=F32, precision=lax.Precision.HIGHEST,
            )
            for n, i in enumerate(range(stop + parts, tiles)):
                z[i] = jnp.where(inside, 0.0, z[i]) - change[n * block:(n + 1) * block]
    yield


def apply_kernel(g_ref, m_ref, o_hbm, r_ref, w_ref, upper, lower, out, sent):
    rows, columns, cols = out.shape
    half = columns // 2
    group = 16
    steps = factor(g_ref, r_ref, w_ref)

    def send(side, i):
        part = pl.ds(side * half, half)
        return pltpu.make_async_copy(out.at[i, part], o_hbm.at[part, i, :], sent)

    def over(side, value, groups, between=None):
        first = 0
        for size in groups:
            for i in range(first, first + size):
                out[i, side * half:(side + 1) * half, :] = value(slice(i * cols, (i + 1) * cols))
                if between:
                    between(i)
            for i in range(first, first + size):
                send(side, i).start()
            first += size

    next(steps)
    high, low = split(w_ref[:half, :])
    upper[...] = jnp.concatenate([high[:, :half], high[:, :half], low[:, :half]], 1)

    def first(at):
        near = m_ref[:half, at]
        right = jnp.concatenate([near, m_ref[columns:columns + half, at], near], 0)
        return jnp.dot(upper[...], right, preferred_element_type=F32)

    over(0, first, (rows,))
    next(steps)
    high, low = split(w_ref[half:, :])
    lower[:half, :columns] = high
    lower[:half, columns:] = high
    lower[half:, :columns] = low
    lower[half:, columns:] = jnp.zeros_like(low)

    def second(at):
        both = jnp.dot(lower[...], m_ref[:, at], preferred_element_type=F32)
        return both[:half] + both[half:]

    over(1, second, (rows // 2, rows // 4, rows // 4))

    pltpu.make_async_copy(out, out, sent).wait()


def apply(total, matrix, rows, cols):
    columns = total.shape[0]
    vmem = pl.BlockSpec(memory_space=pltpu.VMEM)
    return pl.pallas_call(
        apply_kernel,
        out_shape=(
            jax.ShapeDtypeStruct((columns, rows, cols), F32),
            jax.ShapeDtypeStruct((columns, columns), F32),
        ),
        in_specs=[vmem, vmem],
        out_specs=(pl.BlockSpec(memory_space=pltpu.HBM), vmem),
        scratch_shapes=[
            pltpu.VMEM((columns, columns), F32),
            pltpu.VMEM((columns // 2, 3 * columns // 2), BF16),
            pltpu.VMEM((columns, 2 * columns), BF16),
            pltpu.VMEM((rows, columns, cols), F32),
            pltpu.SemaphoreType.DMA,
        ],
        compiler_params=pltpu.CompilerParams(vmem_limit_bytes=20 * 1024 * 1024),
        name="apply",
    )(total, pltpu.with_memory_space_constraint(matrix, pltpu.VMEM))


def on_device(nx, ny, mode_fields, conductance, potential):
    _, rows, cols = mode_fields.shape
    matrix, total = gram(mode_fields, conductance, potential, nx, ny)
    return apply(total, matrix, rows, cols)


def solution(mesh):
    placed = (P(None, "gx", "gy"), P("gx", "gy"), P("gx", "gy"))
    return jax.shard_map(
        functools.partial(on_device, mesh.shape["gx"], mesh.shape["gy"]),
        mesh=mesh, in_specs=placed, out_specs=(P(None, "gx", "gy"), P()), check_vma=False,
    )
```

```python
import functools

import jax
import jax.numpy as jnp
from jax import lax
from jax.experimental import pallas as pl
from jax.experimental.pallas import tpu as pltpu
from jax.sharding import PartitionSpec as P

MESH = pl.DeviceIdType.MESH
F32 = jnp.float32
BF16 = jnp.bfloat16


def split(value):
    high = value.astype(BF16)
    return high, (value - high.astype(F32)).astype(BF16)


def gram_kernel(
    nx, ny, u_hbm, k_hbm, p_hbm, m_ref, g_ref,
    wide, kappa, p_ref, xface, yface, edge, halo, turned, flow, back, acc, part, piece, ring, full,
    load, halo_send, halo_recv, rs_send, rs_recv, all_send, all_recv, ag_send, ag_recv,
):
    rows, cols = k_hbm.shape
    modes = u_hbm.shape[0]
    tiles = cols // 128
    columns = 4 * modes
    share = columns // ny
    px, py = lax.axis_index("gx"), lax.axis_index("gy")

    def fetch(i):
        return pltpu.make_async_copy(u_hbm.at[:, i, :], wide.at[i + 1], load.at[i])

    own = pl.ds(8, rows)
    load_k = pltpu.make_async_copy(k_hbm, kappa.at[own], load.at[rows])
    load_p = pltpu.make_async_copy(p_hbm, p_ref, load.at[rows + 1])

    load_k.start()
    for i in range(rows):
        fetch(i).start()
    load_p.start()
    barrier = pltpu.get_barrier_semaphore()
    for d in range(1, nx):
        pl.semaphore_signal(barrier, inc=1, device_id={"gx": lax.rem(px + d, nx)}, device_id_type=MESH)
    for d in range(1, ny):
        pl.semaphore_signal(barrier, inc=1, device_id={"gy": lax.rem(py + d, ny)}, device_id_type=MESH)

    def iota(height):
        return lax.broadcasted_iota(jnp.int32, (height, 128), 1)

    lanes = iota(modes)
    packed = iota(modes + 8)
    holder = ((packed + 1) & 127) >> 1
    load_k.wait()

    def collect(q, pack):
        for s in range(16):
            fetch(q * 16 + s).wait()
        for s in range(16):
            i = q * 16 + s
            k_row = jnp.broadcast_to(kappa[pl.ds(i + 8, 1), :], (8, cols))
            first = jnp.concatenate([wide[i + 1, :, :128], k_row[:, :128]], 0)
            last = jnp.concatenate([wide[i + 1, :, cols - 128:], k_row[:, cols - 128:]], 0)
            pack = jnp.where(holder == i, pltpu.roll(jnp.where(packed == 0, first, last), 2 * i, 1), pack)
        return pack

    edge[...] = lax.fori_loop(0, rows // 16, collect, jnp.zeros((modes + 8, 128), F32))

    pl.semaphore_wait(barrier, nx + ny - 2)
    has_up, has_down, has_left, has_right = px > 0, px < nx - 1, py > 0, py < ny - 1
    down, up = {"gx": lax.rem(px + 1, nx)}, {"gx": lax.rem(px + nx - 1, nx)}
    right, left = {"gy": lax.rem(py + 1, ny)}, {"gy": lax.rem(py + ny - 1, ny)}
    moves = (
        (wide.at[rows], wide.at[0], down, has_down, has_up),
        (kappa.at[pl.ds(rows, 8)], kappa.at[pl.ds(0, 8)], down, has_down, has_up),
        (wide.at[1], wide.at[rows + 1], up, has_up, has_down),
        (kappa.at[pl.ds(8, 8)], kappa.at[pl.ds(rows + 8, 8)], up, has_up, has_down),
        (edge, halo.at[0], right, has_right, has_left),
        (edge, halo.at[1], left, has_left, has_right),
    )
    copies = [
        (
            pltpu.make_async_remote_copy(
                src_ref=src, dst_ref=dst, send_sem=halo_send.at[n], recv_sem=halo_recv.at[n],
                device_id=device, device_id_type=MESH,
            ), sends, receives,
        )
        for n, (src, dst, device, sends, receives) in enumerate(moves)
    ]
    for copy, sends, _ in copies:
        @pl.when(sends)
        def _():
            copy.start()

    def put(block, i, value):
        high, low = split(value)
        at = pl.ds(pl.multiple_of(i * cols, cols), cols)
        m_ref[block * modes:(block + 1) * modes, at] = high
        m_ref[columns + block * modes:columns + (block + 1) * modes, at] = low

    def flux(i):
        return xface[pl.ds(i, 1), :] * (wide[i] - wide[i + 1])

    xface[pl.ds(1, rows - 1), :] = 0.5 * (kappa[pl.ds(8, rows - 1), :] + kappa[pl.ds(9, rows - 1), :])
    lane = iota(rows)

    def tile(t):
        return slice(t * 128, (t + 1) * 128)

    k_tile = [kappa[own, t * 128:(t + 1) * 128] for t in range(tiles)]
    k_next = [pltpu.roll(k, 127, 1) for k in k_tile]
    for t in range(tiles):
        face = 0.5 * (k_tile[t] + (jnp.where(lane == 127, k_next[t + 1], k_next[t]) if t + 1 < tiles else k_next[t]))
        yface[:, t * 128:(t + 1) * 128] = face if t + 1 < tiles else jnp.where(lane == 127, 0.0, face)
    load_p.wait()

    def local(i):
        center = wide[i + 1]
        put(0, i, center)
        put(3, i, p_ref[pl.ds(i, 1), :] * center)
        for t in range(tiles):
            turned[i, :, tile(t)] = pltpu.roll(center[:, tile(t)], 127, 1)

    def stream(g, _):
        for s in range(group):
            i = g * group + s
            scale = yface[pl.ds(i, 1), :]
            r = [turned[i, :, tile(t)] for t in range(tiles)]
            for t in range(tiles):
                after = jnp.where(lanes == 127, r[t + 1], r[t]) if t + 1 < tiles else r[t]
                f = scale[:, tile(t)] * (wide[i + 1, :, tile(t)] - after)
                flow[i, :, tile(t)] = f
                back[i, :, tile(t)] = pltpu.roll(f, 1, 1)
        return 0

    group = 16

    def inner(first, count, before):
        for s in range(group):
            local(first + s)
            if s < count:
                after = flux(first + s + 2)
                put(1, first + s + 1, after - before)
                before = after
        return before

    def sweep(g, before):
        return inner(g * group, group, before)

    inner(rows - group, group - 2, lax.fori_loop(0, rows // group - 1, sweep, flux(1)))
    lax.fori_loop(0, rows // group, stream, 0)

    for copy, sends, receives in copies:
        @pl.when(sends)
        def _():
            copy.wait_send()

        @pl.when(receives)
        def _():
            copy.wait_recv()

    @pl.when(px == 0)
    def _():
        wide[0] = jnp.zeros((modes, cols), F32)
        kappa[pl.ds(0, 8), :] = jnp.zeros((8, cols), F32)

    @pl.when(px == nx - 1)
    def _():
        wide[rows + 1] = jnp.zeros((modes, cols), F32)
        kappa[pl.ds(rows + 8, 8), :] = jnp.zeros((8, cols), F32)

    @pl.when(py == 0)
    def _():
        halo[0] = jnp.zeros((modes + 8, 128), F32)

    @pl.when(py == ny - 1)
    def _():
        halo[1] = jnp.zeros((modes + 8, 128), F32)

    for i in (0, rows):
        xface[i:i + 1, :] = 0.5 * (kappa[i + 7:i + 8, :] + kappa[i + 8:i + 9, :])
    for i in (0, rows - 1):
        put(1, i, flux(i + 1) - flux(i))
    mine = edge[...]
    other = jnp.where((packed & 1) == 0, pltpu.roll(halo[0], 1, 1), pltpu.roll(halo[1], 127, 1))
    across = 0.5 * (mine[modes:modes + 1] + other[modes:modes + 1]) * (mine[:modes] - other[:modes])

    acc[...] = jnp.zeros_like(acc)

    def build(g, _):
        for s in range(32):
            i = g * 32 + s
            turn = pltpu.roll(across, (128 - 2 * i) & 127, 1)
            b = [back[i, :, tile(t)] for t in range(tiles)]
            y = [flow[i, :, tile(t)] - jnp.where(lanes == 0, b[t - 1], b[t]) for t in range(tiles)]
            y[0] = y[0] + jnp.where(lanes == 0, turn, 0.0)
            y[-1] = y[-1] + jnp.where(lanes == 127, turn, 0.0)
            put(2, i, jnp.concatenate(y, 1))
        at = pl.ds(pl.multiple_of(g * 32 * cols, 32 * cols), 32 * cols)
        acc[...] += lax.dot_general(
            m_ref[:, at], m_ref[:columns, at], (((1,), (1,)), ((), ())), preferred_element_type=F32
        )
        return 0

    lax.fori_loop(0, rows // 32, build, 0)
    cross = acc[columns:]
    total = (acc[:columns] + (cross + cross.T)) * (1.0 / (rows * cols * nx * ny))
    for j in range(ny):
        part[j] = total[j * share:(j + 1) * share]

    copies = [
        pltpu.make_async_remote_copy(
            src_ref=part.at[lax.rem(py + d, ny)], dst_ref=piece.at[py], send_sem=rs_send.at[d], recv_sem=rs_recv.at[d],
            device_id={"gy": lax.rem(py + d, ny)}, device_id_type=MESH,
        )
        for d in range(1, ny)
    ]
    for copy in copies:
        copy.start()
    piece[py] = part[py]
    for copy in copies:
        copy.wait()
    ring[px] = functools.reduce(jnp.add, [piece[j] for j in range(ny)])

    copies = [
        pltpu.make_async_remote_copy(
            src_ref=ring.at[px], dst_ref=ring.at[px], send_sem=all_send.at[d], recv_sem=all_recv.at[d],
            device_id={"gx": lax.rem(px + d, nx)}, device_id_type=MESH,
        )
        for d in range(1, nx)
    ]
    for copy in copies:
        copy.start()
    for copy in copies:
        copy.wait()
    full[py] = functools.reduce(jnp.add, [ring[j] for j in range(nx)])

    copies = [
        pltpu.make_async_remote_copy(
            src_ref=full.at[py], dst_ref=full.at[py], send_sem=ag_send.at[d], recv_sem=ag_recv.at[d],
            device_id={"gy": lax.rem(py + d, ny)}, device_id_type=MESH,
        )
        for d in range(1, ny)
    ]
    for copy in copies:
        copy.start()
    for copy in copies:
        copy.wait()
    for j in range(ny):
        g_ref[j * share:(j + 1) * share, :] = full[j]


def gram(fields, conduct, potential, nx, ny):
    modes, rows, cols = fields.shape
    columns = 4 * modes
    vmem = pl.BlockSpec(memory_space=pltpu.VMEM)
    dma = pltpu.SemaphoreType.DMA
    return pl.pallas_call(
        functools.partial(gram_kernel, nx, ny),
        out_shape=(
            pltpu.VMEM((2 * columns, rows * cols), BF16),
            pltpu.VMEM((columns, columns), F32),
        ),
        in_specs=[pl.BlockSpec(memory_space=pltpu.HBM)] * 3,
        out_specs=(vmem, vmem),
        scratch_shapes=[
            pltpu.VMEM((rows + 2, modes, cols), F32),
            pltpu.VMEM((rows + 16, cols), F32),
            pltpu.VMEM((rows, cols), F32),
            pltpu.VMEM((rows + 8, cols), F32),
            pltpu.VMEM((rows, cols), F32),
            pltpu.VMEM((modes + 8, 128), F32),
            pltpu.VMEM((2, modes + 8, 128), F32),
            pltpu.VMEM((rows, modes, cols), F32),
            pltpu.VMEM((rows, modes, cols), F32),
            pltpu.VMEM((rows, modes, cols), F32),
            pltpu.VMEM((2 * columns, columns), F32),
            pltpu.VMEM((ny, columns // ny, columns), F32),
            pltpu.VMEM((ny, columns // ny, columns), F32),
            pltpu.VMEM((nx, columns // ny, columns), F32),
            pltpu.VMEM((ny, columns // ny, columns), F32),
            dma((rows + 2,)),
            dma((6,)), dma((6,)), dma((ny,)), dma((ny,)), dma((nx,)), dma((nx,)), dma((ny,)), dma((ny,)),
        ],
        compiler_params=pltpu.CompilerParams(
            collective_id=0, has_side_effects=True, vmem_limit_bytes=28 * 1024 * 1024
        ),
        name="gram",
    )(*(pltpu.with_memory_space_constraint(a, pltpu.HBM) for a in (fields, conduct, potential)))


def factor(g_ref, r_ref, w_ref):
    size = g_ref.shape[0]
    block, width = 8, 16
    parts, tiles = width // block, size // block
    lane = lax.broadcasted_iota(jnp.int32, (block, size), 1)
    sub = lax.broadcasted_iota(jnp.int32, (block, size), 0)

    def row(value, j):
        return jnp.broadcast_to(value[j:j + 1], (block, size))

    def column(value, j):
        return jnp.broadcast_to(value[:, j:j + 1], (block, size))

    z = [g_ref[i * block:(i + 1) * block, :] for i in range(tiles)]
    for at in range(0, size, width):
        if at == size // 2:
            yield
        start = at // block
        stop = start + parts
        inside = (lane >= at) & (lane < at + width)
        cols = [[column(value, at + k) for value in z[start:stop]] for k in range(width)]
        plain = z[start:stop]
        swept = [
            jnp.where(inside, jnp.where(lane == at + h * block + sub, 1.0, 0.0), value)
            for h, value in enumerate(plain)
        ]
        solved = [jnp.zeros((block, size), F32)] * parts
        upper = list(solved)
        for j in range(width):
            h, s = divmod(j, block)
            root = lax.rsqrt(row(cols[j][h], s))
            low = [value * root for value in cols[j]]
            both = list(low)
            both[h] = jnp.where(sub == s, -root, low[h])

            def sweep(values, line):
                return [
                    (jnp.where(sub == s, 0.0, value) if q == h else value) - both[q] * line
                    for q, value in enumerate(values)
                ]

            for k in range(j + 1, width):
                cols[k] = sweep(cols[k], row(low[k // block], k % block))
            line = row(swept[h], s) * root
            solved[h] = jnp.where(sub == s, line, solved[h])
            swept = sweep(swept, line)
            line = row(plain[h], s) * root
            upper[h] = jnp.where(sub == s, line, upper[h])
            plain = [value if q < h else value - low[q] * line for q, value in enumerate(plain)]
        for h in range(parts):
            first = at + h * block
            r_ref[first:first + block, :] = jnp.where(lane >= first + sub, upper[h], 0.0)
            w_ref[first:first + block, :] = jnp.where(lane <= first + sub, solved[h], 0.0)
        for i in range(stop, min(stop + parts, tiles)):
            terms = [column(z[i], at + k) * row(swept[k // block], k % block) for k in range(width)]
            while len(terms) > 1:
                terms = [x + y for x, y in zip(terms[::2], terms[1::2])]
            z[i] = jnp.where(inside, 0.0, z[i]) - terms[0]
        if stop + parts < tiles:
            pads = [jnp.zeros((at, size), F32)] * (at > 0)
            sides = jnp.concatenate(pads + swept + [jnp.zeros((size - at - width, size), F32)], 0)
            change = jnp.dot(
                jnp.concatenate(z[stop + parts:], 0), sides,
                preferred_element_type=F32, precision=lax.Precision.HIGHEST,
            )
            for n, i in enumerate(range(stop + parts, tiles)):
                z[i] = jnp.where(inside, 0.0, z[i]) - change[n * block:(n + 1) * block]
    yield


def apply_kernel(g_ref, m_ref, o_hbm, r_hbm, r_ref, w_ref, upper, lower, out, sent, kept):
    rows, columns, cols = out.shape
    half = columns // 2
    group = 16
    steps = factor(g_ref, r_ref, w_ref)

    def send(side, i):
        part = pl.ds(side * half, half)
        return pltpu.make_async_copy(out.at[i, part], o_hbm.at[part, i, :], sent)

    def over(side, value, groups, between=None):
        first = 0
        for size in groups:
            for i in range(first, first + size):
                out[i, side * half:(side + 1) * half, :] = value(slice(i * cols, (i + 1) * cols))
                if between:
                    between(i)
            for i in range(first, first + size):
                send(side, i).start()
            first += size

    next(steps)
    high, low = split(w_ref[:half, :])
    upper[...] = jnp.concatenate([high[:, :half], high[:, :half], low[:, :half]], 1)

    def first(at):
        near = m_ref[:half, at]
        right = jnp.concatenate([near, m_ref[columns:columns + half, at], near], 0)
        return jnp.dot(upper[...], right, preferred_element_type=F32)

    over(0, first, (rows,))
    next(steps)
    keep = pltpu.make_async_copy(r_ref, r_hbm, kept)
    keep.start()
    high, low = split(w_ref[half:, :])
    lower[:half, :columns] = high
    lower[:half, columns:] = high
    lower[half:, :columns] = low
    lower[half:, columns:] = jnp.zeros_like(low)

    def second(at):
        both = jnp.dot(lower[...], m_ref[:, at], preferred_element_type=F32)
        return both[:half] + both[half:]

    over(1, second, (rows // 2, rows // 4, rows // 4))

    keep.wait()
    pltpu.make_async_copy(out, out, sent).wait()


def apply(total, matrix, rows, cols):
    columns = total.shape[0]
    vmem = pl.BlockSpec(memory_space=pltpu.VMEM)
    return pl.pallas_call(
        apply_kernel,
        out_shape=(
            jax.ShapeDtypeStruct((columns, rows, cols), F32),
            jax.ShapeDtypeStruct((columns, columns), F32),
        ),
        in_specs=[vmem, vmem],
        out_specs=(pl.BlockSpec(memory_space=pltpu.HBM),) * 2,
        scratch_shapes=[
            pltpu.VMEM((columns, columns), F32),
            pltpu.VMEM((columns, columns), F32),
            pltpu.VMEM((columns // 2, 3 * columns // 2), BF16),
            pltpu.VMEM((columns, 2 * columns), BF16),
            pltpu.VMEM((rows, columns, cols), F32),
            pltpu.SemaphoreType.DMA,
            pltpu.SemaphoreType.DMA,
        ],
        compiler_params=pltpu.CompilerParams(vmem_limit_bytes=20 * 1024 * 1024),
        name="apply",
    )(total, pltpu.with_memory_space_constraint(matrix, pltpu.VMEM))


def on_device(nx, ny, mode_fields, conductance, potential):
    _, rows, cols = mode_fields.shape
    matrix, total = gram(mode_fields, conductance, potential, nx, ny)
    return apply(total, matrix, rows, cols)


def solution(mesh):
    placed = (P(None, "gx", "gy"), P("gx", "gy"), P("gx", "gy"))
    return jax.shard_map(
        functools.partial(on_device, mesh.shape["gx"], mesh.shape["gy"]),
        mesh=mesh, in_specs=placed, out_specs=(P(None, "gx", "gy"), P()), check_vma=False,
    )
```

```python
import functools

import jax
import jax.numpy as jnp
from jax import lax
from jax.experimental import pallas as pl
from jax.experimental.pallas import tpu as pltpu
from jax.sharding import PartitionSpec as P

MESH = pl.DeviceIdType.MESH
F32 = jnp.float32
BF16 = jnp.bfloat16


def split(value):
    high = value.astype(BF16)
    return high, (value - high.astype(F32)).astype(BF16)


def gram_kernel(
    nx, ny, u_hbm, k_hbm, p_hbm, m_ref, g_ref,
    wide, kappa, p_ref, xface, yface, edge, halo, turned, flow, back, acc, part, piece, ring, full,
    load, halo_send, halo_recv, rs_send, rs_recv, all_send, all_recv, ag_send, ag_recv,
):
    rows, cols = k_hbm.shape
    modes = u_hbm.shape[0]
    tiles = cols // 128
    columns = 4 * modes
    share = 3 * columns // 4 // ny
    px, py = lax.axis_index("gx"), lax.axis_index("gy")

    def fetch(i):
        return pltpu.make_async_copy(u_hbm.at[:, i, :], wide.at[i + 1], load.at[i])

    own = pl.ds(8, rows)
    load_k = pltpu.make_async_copy(k_hbm, kappa.at[own], load.at[rows])
    load_p = pltpu.make_async_copy(p_hbm, p_ref, load.at[rows + 1])

    load_k.start()
    for i in range(rows):
        fetch(i).start()
    load_p.start()
    barrier = pltpu.get_barrier_semaphore()
    for d in range(1, nx):
        pl.semaphore_signal(barrier, inc=1, device_id={"gx": lax.rem(px + d, nx)}, device_id_type=MESH)
    for d in range(1, ny):
        pl.semaphore_signal(barrier, inc=1, device_id={"gy": lax.rem(py + d, ny)}, device_id_type=MESH)

    def iota(height):
        return lax.broadcasted_iota(jnp.int32, (height, 128), 1)

    lanes = iota(modes)
    packed = iota(modes + 8)
    holder = ((packed + 1) & 127) >> 1
    load_k.wait()

    def collect(q, pack):
        for s in range(16):
            fetch(q * 16 + s).wait()
        for s in range(16):
            i = q * 16 + s
            k_row = jnp.broadcast_to(kappa[pl.ds(i + 8, 1), :], (8, cols))
            first = jnp.concatenate([wide[i + 1, :, :128], k_row[:, :128]], 0)
            last = jnp.concatenate([wide[i + 1, :, cols - 128:], k_row[:, cols - 128:]], 0)
            pack = jnp.where(holder == i, pltpu.roll(jnp.where(packed == 0, first, last), 2 * i, 1), pack)
        return pack

    edge[...] = lax.fori_loop(0, rows // 16, collect, jnp.zeros((modes + 8, 128), F32))

    pl.semaphore_wait(barrier, nx + ny - 2)
    has_up, has_down, has_left, has_right = px > 0, px < nx - 1, py > 0, py < ny - 1
    down, up = {"gx": lax.rem(px + 1, nx)}, {"gx": lax.rem(px + nx - 1, nx)}
    right, left = {"gy": lax.rem(py + 1, ny)}, {"gy": lax.rem(py + ny - 1, ny)}
    moves = (
        (wide.at[rows], wide.at[0], down, has_down, has_up),
        (kappa.at[pl.ds(rows, 8)], kappa.at[pl.ds(0, 8)], down, has_down, has_up),
        (wide.at[1], wide.at[rows + 1], up, has_up, has_down),
        (kappa.at[pl.ds(8, 8)], kappa.at[pl.ds(rows + 8, 8)], up, has_up, has_down),
        (edge, halo.at[0], right, has_right, has_left),
        (edge, halo.at[1], left, has_left, has_right),
    )
    copies = [
        (
            pltpu.make_async_remote_copy(
                src_ref=src, dst_ref=dst, send_sem=halo_send.at[n], recv_sem=halo_recv.at[n],
                device_id=device, device_id_type=MESH,
            ), sends, receives,
        )
        for n, (src, dst, device, sends, receives) in enumerate(moves)
    ]
    for copy, sends, _ in copies:
        @pl.when(sends)
        def _():
            copy.start()

    def put(block, i, value):
        high, low = split(value)
        at = slice(i * cols, (i + 1) * cols) if isinstance(i, int) else pl.ds(pl.multiple_of(i * cols, cols), cols)
        m_ref[block * modes:(block + 1) * modes, at] = high
        m_ref[columns + block * modes:columns + (block + 1) * modes, at] = low

    def flux(i):
        return xface[pl.ds(i, 1), :] * (wide[i] - wide[i + 1])

    xface[pl.ds(1, rows - 1), :] = 0.5 * (kappa[pl.ds(8, rows - 1), :] + kappa[pl.ds(9, rows - 1), :])
    lane = iota(rows)

    def tile(t):
        return slice(t * 128, (t + 1) * 128)

    k_tile = [kappa[own, t * 128:(t + 1) * 128] for t in range(tiles)]
    k_next = [pltpu.roll(k, 127, 1) for k in k_tile]
    for t in range(tiles):
        face = 0.5 * (k_tile[t] + (jnp.where(lane == 127, k_next[t + 1], k_next[t]) if t + 1 < tiles else k_next[t]))
        yface[:, t * 128:(t + 1) * 128] = face if t + 1 < tiles else jnp.where(lane == 127, 0.0, face)
    load_p.wait()

    def local(i):
        center = wide[i + 1]
        put(0, i, center)
        put(3, i, p_ref[pl.ds(i, 1), :] * center)
        for t in range(tiles):
            turned[i, :, tile(t)] = pltpu.roll(center[:, tile(t)], 127, 1)

    def stream(g, _):
        for s in range(group):
            i = g * group + s
            scale = yface[pl.ds(i, 1), :]
            r = [turned[i, :, tile(t)] for t in range(tiles)]
            for t in range(tiles):
                after = jnp.where(lanes == 127, r[t + 1], r[t]) if t + 1 < tiles else r[t]
                f = scale[:, tile(t)] * (wide[i + 1, :, tile(t)] - after)
                flow[i, :, tile(t)] = f
                back[i, :, tile(t)] = pltpu.roll(f, 1, 1)
        return 0

    group = 16

    def inner(first, count, before):
        for s in range(group):
            local(first + s)
            if s < count:
                after = flux(first + s + 2)
                put(1, first + s + 1, after - before)
                before = after
        return before

    def sweep(g, before):
        return inner(g * group, group, before)

    inner(rows - group, group - 2, lax.fori_loop(0, rows // group - 1, sweep, flux(1)))
    lax.fori_loop(0, rows // group, stream, 0)

    def settle(some):
        for copy, sends, receives in some:
            @pl.when(sends)
            def _():
                copy.wait_send()

            @pl.when(receives)
            def _():
                copy.wait_recv()

    settle(copies[4:])

    @pl.when(py == 0)
    def _():
        halo[0] = jnp.zeros((modes + 8, 128), F32)

    @pl.when(py == ny - 1)
    def _():
        halo[1] = jnp.zeros((modes + 8, 128), F32)

    mine = edge[...]
    other = jnp.where((packed & 1) == 0, pltpu.roll(halo[0], 1, 1), pltpu.roll(halo[1], 127, 1))
    border = 0.5 * (mine[modes:modes + 1] + other[modes:modes + 1]) * (mine[:modes] - other[:modes])

    quarter = rows // 4
    acc[...] = jnp.zeros_like(acc)

    def edges():
        settle(copies[:4])

        @pl.when(px == 0)
        def _():
            wide[0] = jnp.zeros((modes, cols), F32)
            kappa[pl.ds(0, 8), :] = jnp.zeros((8, cols), F32)

        @pl.when(px == nx - 1)
        def _():
            wide[rows + 1] = jnp.zeros((modes, cols), F32)
            kappa[pl.ds(rows + 8, 8), :] = jnp.zeros((8, cols), F32)

        for i in (0, rows):
            xface[i:i + 1, :] = 0.5 * (kappa[i + 7:i + 8, :] + kappa[i + 8:i + 9, :])
        for i in (0, rows - 1):
            put(1, i, flux(i + 1) - flux(i))

    def build(g, _):
        pl.when(g == 1)(edges)
        starts = [(2 * g + 1) * quarter, lax.rem(2 * g + 2, 4) * quarter]
        for first in starts:
            for s in range(quarter):
                i = first + s
                turn = pltpu.roll(border, (128 - 2 * i) & 127, 1)
                b = [back[i, :, tile(t)] for t in range(tiles)]
                y = [flow[i, :, tile(t)] - jnp.where(lanes == 0, b[t - 1], b[t]) for t in range(tiles)]
                y[0] = y[0] + jnp.where(lanes == 0, turn, 0.0)
                y[-1] = y[-1] + jnp.where(lanes == 127, turn, 0.0)
                put(2, i, jnp.concatenate(y, 1))
        for first in starts:
            at = pl.ds(pl.multiple_of(first * cols, quarter * cols), quarter * cols)
            acc[...] += lax.dot_general(
                m_ref[:, at], m_ref[:columns, at], (((1,), (1,)), ((), ())), preferred_element_type=F32
            )
        return 0

    lax.fori_loop(0, 2, build, 0)
    half = columns // 2
    cross = acc[columns:]
    scale = 1.0 / (rows * cols * nx * ny)
    upper = (acc[:half] + (cross[:half] + cross[:, :half].T)) * scale
    corner = cross[half:, half:]
    corner = (acc[half:columns, half:] + (corner + corner.T)) * scale
    total = jnp.concatenate([upper, jnp.concatenate([corner[half // 2:], corner[:half // 2]], 1)], 0)
    for j in range(ny):
        part[j] = total[j * share:(j + 1) * share]

    copies = [
        pltpu.make_async_remote_copy(
            src_ref=part.at[lax.rem(py + d, ny)], dst_ref=piece.at[py], send_sem=rs_send.at[d], recv_sem=rs_recv.at[d],
            device_id={"gy": lax.rem(py + d, ny)}, device_id_type=MESH,
        )
        for d in range(1, ny)
    ]
    for copy in copies:
        copy.start()
    piece[py] = part[py]
    for copy in copies:
        copy.wait()
    ring[px] = functools.reduce(jnp.add, [piece[j] for j in range(ny)])

    copies = [
        pltpu.make_async_remote_copy(
            src_ref=ring.at[px], dst_ref=ring.at[px], send_sem=all_send.at[d], recv_sem=all_recv.at[d],
            device_id={"gx": lax.rem(px + d, nx)}, device_id_type=MESH,
        )
        for d in range(1, nx)
    ]
    for copy in copies:
        copy.start()
    for copy in copies:
        copy.wait()
    full[py] = functools.reduce(jnp.add, [ring[j] for j in range(nx)])

    copies = [
        pltpu.make_async_remote_copy(
            src_ref=full.at[py], dst_ref=full.at[py], send_sem=ag_send.at[d], recv_sem=ag_recv.at[d],
            device_id={"gy": lax.rem(py + d, ny)}, device_id_type=MESH,
        )
        for d in range(1, ny)
    ]
    for copy in copies:
        copy.start()
    for copy in copies:
        copy.wait()
    whole = jnp.concatenate([full[j] for j in range(ny)], 0)
    upper = whole[:half]
    corner = jnp.concatenate([whole[half:, half:], whole[half:, :half]], 0)
    g_ref[:half, :] = upper
    g_ref[half:, :] = jnp.concatenate([upper[:, half:].T, corner], 1)


def gram(fields, conduct, potential, nx, ny):
    modes, rows, cols = fields.shape
    columns = 4 * modes
    share = 3 * columns // 4 // ny
    vmem = pl.BlockSpec(memory_space=pltpu.VMEM)
    dma = pltpu.SemaphoreType.DMA
    return pl.pallas_call(
        functools.partial(gram_kernel, nx, ny),
        out_shape=(
            pltpu.VMEM((2 * columns, rows * cols), BF16),
            pltpu.VMEM((columns, columns), F32),
        ),
        in_specs=[pl.BlockSpec(memory_space=pltpu.HBM)] * 3,
        out_specs=(vmem, vmem),
        scratch_shapes=[
            pltpu.VMEM((rows + 2, modes, cols), F32),
            pltpu.VMEM((rows + 16, cols), F32),
            pltpu.VMEM((rows, cols), F32),
            pltpu.VMEM((rows + 8, cols), F32),
            pltpu.VMEM((rows, cols), F32),
            pltpu.VMEM((modes + 8, 128), F32),
            pltpu.VMEM((2, modes + 8, 128), F32),
            pltpu.VMEM((rows, modes, cols), F32),
            pltpu.VMEM((rows, modes, cols), F32),
            pltpu.VMEM((rows, modes, cols), F32),
            pltpu.VMEM((2 * columns, columns), F32),
            pltpu.VMEM((ny, share, columns), F32),
            pltpu.VMEM((ny, share, columns), F32),
            pltpu.VMEM((nx, share, columns), F32),
            pltpu.VMEM((ny, share, columns), F32),
            dma((rows + 2,)),
            dma((6,)), dma((6,)), dma((ny,)), dma((ny,)), dma((nx,)), dma((nx,)), dma((ny,)), dma((ny,)),
        ],
        compiler_params=pltpu.CompilerParams(
            collective_id=0, has_side_effects=True, vmem_limit_bytes=28 * 1024 * 1024
        ),
        name="gram",
    )(*(pltpu.with_memory_space_constraint(a, pltpu.HBM) for a in (fields, conduct, potential)))


def factor(g_ref, r_ref, w_ref):
    size = g_ref.shape[0]
    block, width = 8, 16
    parts, tiles = width // block, size // block
    lane = lax.broadcasted_iota(jnp.int32, (block, size), 1)
    sub = lax.broadcasted_iota(jnp.int32, (block, size), 0)

    def row(value, j):
        return jnp.broadcast_to(value[j:j + 1], (block, size))

    def column(value, j):
        return jnp.broadcast_to(value[:, j:j + 1], (block, size))

    z = [g_ref[i * block:(i + 1) * block, :] for i in range(tiles)]
    for at in range(0, size, width):
        if at == size // 2:
            yield
        start = at // block
        stop = start + parts
        inside = (lane >= at) & (lane < at + width)
        cols = [[column(value, at + k) for value in z[start:stop]] for k in range(width)]
        plain = z[start:stop]
        swept = [
            jnp.where(inside, jnp.where(lane == at + h * block + sub, 1.0, 0.0), value)
            for h, value in enumerate(plain)
        ]
        solved = [jnp.zeros((block, size), F32)] * parts
        upper = list(solved)
        for j in range(width):
            h, s = divmod(j, block)
            root = lax.rsqrt(row(cols[j][h], s))
            low = [value * root for value in cols[j]]
            both = list(low)
            both[h] = jnp.where(sub == s, -root, low[h])

            def sweep(values, line):
                return [
                    (jnp.where(sub == s, 0.0, value) if q == h else value) - both[q] * line
                    for q, value in enumerate(values)
                ]

            for k in range(j + 1, width):
                cols[k] = sweep(cols[k], row(low[k // block], k % block))
            line = row(swept[h], s) * root
            solved[h] = jnp.where(sub == s, line, solved[h])
            swept = sweep(swept, line)
            line = row(plain[h], s) * root
            upper[h] = jnp.where(sub == s, line, upper[h])
            plain = [value if q < h else value - low[q] * line for q, value in enumerate(plain)]
            if at >= size // 2:
                yield
        for h in range(parts):
            first = at + h * block
            r_ref[first:first + block, :] = jnp.where(lane >= first + sub, upper[h], 0.0)
            w_ref[first:first + block, :] = jnp.where(lane <= first + sub, solved[h], 0.0)
        for i in range(stop, min(stop + parts, tiles)):
            terms = [column(z[i], at + k) * row(swept[k // block], k % block) for k in range(width)]
            while len(terms) > 1:
                terms = [x + y for x, y in zip(terms[::2], terms[1::2])]
            z[i] = jnp.where(inside, 0.0, z[i]) - terms[0]
        if stop + parts < tiles:
            pads = [jnp.zeros((at, size), F32)] * (at > 0)
            sides = jnp.concatenate(pads + swept + [jnp.zeros((size - at - width, size), F32)], 0)
            change = jnp.dot(
                jnp.concatenate(z[stop + parts:], 0), sides,
                preferred_element_type=F32, precision=lax.Precision.HIGHEST,
            )
            for n, i in enumerate(range(stop + parts, tiles)):
                z[i] = jnp.where(inside, 0.0, z[i]) - change[n * block:(n + 1) * block]
    yield


def apply_kernel(g_ref, m_ref, o_hbm, r_hbm, r_ref, w_ref, upper, lower, out, sent, kept):
    rows, columns, cols = out.shape
    half = columns // 2
    group = 16
    steps = factor(g_ref, r_ref, w_ref)

    def send(side, i):
        part = pl.ds(side * half, half)
        return pltpu.make_async_copy(out.at[i, part], o_hbm.at[part, i, :], sent)

    def over(side, value, groups, between=None):
        first = 0
        for size in groups:
            for i in range(first, first + size):
                out[i, side * half:(side + 1) * half, :] = value(slice(i * cols, (i + 1) * cols))
                if between:
                    between(i)
            for i in range(first, first + size):
                send(side, i).start()
            first += size

    next(steps)
    high, low = split(w_ref[:half, :])
    upper[...] = jnp.concatenate([high[:, :half], high[:, :half], low[:, :half]], 1)

    def first(at):
        near = m_ref[:half, at]
        right = jnp.concatenate([near, m_ref[columns:columns + half, at], near], 0)
        return jnp.dot(upper[...], right, preferred_element_type=F32)

    def advance(i):
        if i >= rows // 2:
            next(steps)
            next(steps)

    over(0, first, (rows // 2, rows // 2), advance)
    for _ in steps:
        pass
    keep = pltpu.make_async_copy(r_ref, r_hbm, kept)
    keep.start()
    high, low = split(w_ref[half:, :])
    lower[:half, :columns] = high
    lower[:half, columns:] = high
    lower[half:, :columns] = low
    lower[half:, columns:] = jnp.zeros_like(low)

    def second(at):
        both = jnp.dot(lower[...], m_ref[:, at], preferred_element_type=F32)
        return both[:half] + both[half:]

    over(1, second, (rows // 2, rows // 4, rows // 4))

    keep.wait()
    pltpu.make_async_copy(out, out, sent).wait()


def apply(total, matrix, rows, cols):
    columns = total.shape[0]
    vmem = pl.BlockSpec(memory_space=pltpu.VMEM)
    return pl.pallas_call(
        apply_kernel,
        out_shape=(
            jax.ShapeDtypeStruct((columns, rows, cols), F32),
            jax.ShapeDtypeStruct((columns, columns), F32),
        ),
        in_specs=[vmem, vmem],
        out_specs=(pl.BlockSpec(memory_space=pltpu.HBM),) * 2,
        scratch_shapes=[
            pltpu.VMEM((columns, columns), F32),
            pltpu.VMEM((columns, columns), F32),
            pltpu.VMEM((columns // 2, 3 * columns // 2), BF16),
            pltpu.VMEM((columns, 2 * columns), BF16),
            pltpu.VMEM((rows, columns, cols), F32),
            pltpu.SemaphoreType.DMA,
            pltpu.SemaphoreType.DMA,
        ],
        compiler_params=pltpu.CompilerParams(vmem_limit_bytes=20 * 1024 * 1024),
        name="apply",
    )(total, pltpu.with_memory_space_constraint(matrix, pltpu.VMEM))


def on_device(nx, ny, mode_fields, conductance, potential):
    _, rows, cols = mode_fields.shape
    matrix, total = gram(mode_fields, conductance, potential, nx, ny)
    return apply(total, matrix, rows, cols)


def solution(mesh):
    placed = (P(None, "gx", "gy"), P("gx", "gy"), P("gx", "gy"))
    return jax.shard_map(
        functools.partial(on_device, mesh.shape["gx"], mesh.shape["gy"]),
        mesh=mesh, in_specs=placed, out_specs=(P(None, "gx", "gy"), P()), check_vma=False,
    )
```

```python
import functools

import jax
import jax.numpy as jnp
from jax import lax
from jax.experimental import pallas as pl
from jax.experimental.pallas import tpu as pltpu
from jax.sharding import PartitionSpec as P

MESH = pl.DeviceIdType.MESH
F32 = jnp.float32
BF16 = jnp.bfloat16


def split(value):
    high = value.astype(BF16)
    return high, (value - high.astype(F32)).astype(BF16)


def gram_kernel(
    nx, ny, u_hbm, k_hbm, p_hbm, m_ref, g_ref,
    wide, kappa, p_ref, xface, yface, edge, halo, turned, flow, back, acc, part, piece, ring, full,
    load, halo_send, halo_recv, rs_send, rs_recv, all_send, all_recv, ag_send, ag_recv,
):
    rows, cols = k_hbm.shape
    modes = u_hbm.shape[0]
    tiles = cols // 128
    columns = 4 * modes
    share = 3 * columns // 4 // ny
    px, py = lax.axis_index("gx"), lax.axis_index("gy")

    def fetch(i):
        return pltpu.make_async_copy(u_hbm.at[:, i, :], wide.at[i + 1], load.at[i])

    own = pl.ds(8, rows)
    load_k = pltpu.make_async_copy(k_hbm, kappa.at[own], load.at[rows])
    load_p = pltpu.make_async_copy(p_hbm, p_ref, load.at[rows + 1])

    load_k.start()
    for i in range(rows // 2):
        fetch(i).start()
    barrier = pltpu.get_barrier_semaphore()
    for d in range(1, nx):
        pl.semaphore_signal(barrier, inc=1, device_id={"gx": lax.rem(px + d, nx)}, device_id_type=MESH)
    for d in range(1, ny):
        pl.semaphore_signal(barrier, inc=1, device_id={"gy": lax.rem(py + d, ny)}, device_id_type=MESH)
    for i in range(rows // 2, rows):
        fetch(i).start()
    load_p.start()

    def iota(height):
        return lax.broadcasted_iota(jnp.int32, (height, 128), 1)

    lanes = iota(modes)
    packed = iota(modes + 8)
    holder = ((packed + 1) & 127) >> 1
    load_k.wait()

    def collect(q, pack):
        for s in range(16):
            fetch(q * 16 + s).wait()
        for s in range(16):
            i = q * 16 + s
            k_row = jnp.broadcast_to(kappa[pl.ds(i + 8, 1), :], (8, cols))
            first = jnp.concatenate([wide[i + 1, :, :128], k_row[:, :128]], 0)
            last = jnp.concatenate([wide[i + 1, :, cols - 128:], k_row[:, cols - 128:]], 0)
            pack = jnp.where(holder == i, pltpu.roll(jnp.where(packed == 0, first, last), 2 * i, 1), pack)
        return pack

    edge[...] = lax.fori_loop(0, rows // 16, collect, jnp.zeros((modes + 8, 128), F32))

    pl.semaphore_wait(barrier, nx + ny - 2)
    has_up, has_down, has_left, has_right = px > 0, px < nx - 1, py > 0, py < ny - 1
    down, up = {"gx": lax.rem(px + 1, nx)}, {"gx": lax.rem(px + nx - 1, nx)}
    right, left = {"gy": lax.rem(py + 1, ny)}, {"gy": lax.rem(py + ny - 1, ny)}
    moves = (
        (wide.at[rows], wide.at[0], down, has_down, has_up),
        (kappa.at[pl.ds(rows, 8)], kappa.at[pl.ds(0, 8)], down, has_down, has_up),
        (wide.at[1], wide.at[rows + 1], up, has_up, has_down),
        (kappa.at[pl.ds(8, 8)], kappa.at[pl.ds(rows + 8, 8)], up, has_up, has_down),
        (edge, halo.at[0], right, has_right, has_left),
        (edge, halo.at[1], left, has_left, has_right),
    )
    copies = [
        (
            pltpu.make_async_remote_copy(
                src_ref=src, dst_ref=dst, send_sem=halo_send.at[n], recv_sem=halo_recv.at[n],
                device_id=device, device_id_type=MESH,
            ), sends, receives,
        )
        for n, (src, dst, device, sends, receives) in enumerate(moves)
    ]
    for copy, sends, _ in copies:
        @pl.when(sends)
        def _():
            copy.start()

    def put(block, i, value):
        high, low = split(value)
        at = slice(i * cols, (i + 1) * cols) if isinstance(i, int) else pl.ds(pl.multiple_of(i * cols, cols), cols)
        m_ref[block * modes:(block + 1) * modes, at] = high
        m_ref[columns + block * modes:columns + (block + 1) * modes, at] = low

    def flux(i):
        return xface[pl.ds(i, 1), :] * (wide[i] - wide[i + 1])

    xface[pl.ds(1, rows - 1), :] = 0.5 * (kappa[pl.ds(8, rows - 1), :] + kappa[pl.ds(9, rows - 1), :])
    lane = iota(rows)

    def tile(t):
        return slice(t * 128, (t + 1) * 128)

    k_tile = [kappa[own, t * 128:(t + 1) * 128] for t in range(tiles)]
    k_next = [pltpu.roll(k, 127, 1) for k in k_tile]
    for t in range(tiles):
        face = 0.5 * (k_tile[t] + (jnp.where(lane == 127, k_next[t + 1], k_next[t]) if t + 1 < tiles else k_next[t]))
        yface[:, t * 128:(t + 1) * 128] = face if t + 1 < tiles else jnp.where(lane == 127, 0.0, face)
    load_p.wait()

    def local(i):
        center = wide[i + 1]
        put(0, i, center)
        put(3, i, p_ref[pl.ds(i, 1), :] * center)
        for t in range(tiles):
            turned[i, :, tile(t)] = pltpu.roll(center[:, tile(t)], 127, 1)

    def stream(g, _):
        for s in range(group):
            i = g * group + s
            scale = yface[pl.ds(i, 1), :]
            r = [turned[i, :, tile(t)] for t in range(tiles)]
            for t in range(tiles):
                after = jnp.where(lanes == 127, r[t + 1], r[t]) if t + 1 < tiles else r[t]
                f = scale[:, tile(t)] * (wide[i + 1, :, tile(t)] - after)
                flow[i, :, tile(t)] = f
                back[i, :, tile(t)] = pltpu.roll(f, 1, 1)
        return 0

    group = 32

    def inner(first, count, before):
        for s in range(group):
            local(first + s)
            if s < count:
                after = flux(first + s + 2)
                put(1, first + s + 1, after - before)
                before = after
        return before

    def sweep(g, before):
        return inner(g * group, group, before)

    inner(rows - group, group - 2, lax.fori_loop(0, rows // group - 1, sweep, flux(1)))
    lax.fori_loop(0, rows // group, stream, 0)

    def settle(some):
        for copy, sends, receives in some:
            @pl.when(sends)
            def _():
                copy.wait_send()

            @pl.when(receives)
            def _():
                copy.wait_recv()

    settle(copies[4:])

    @pl.when(py == 0)
    def _():
        halo[0] = jnp.zeros((modes + 8, 128), F32)

    @pl.when(py == ny - 1)
    def _():
        halo[1] = jnp.zeros((modes + 8, 128), F32)

    mine = edge[...]
    other = jnp.where((packed & 1) == 0, pltpu.roll(halo[0], 1, 1), pltpu.roll(halo[1], 127, 1))
    border = 0.5 * (mine[modes:modes + 1] + other[modes:modes + 1]) * (mine[:modes] - other[:modes])

    quarter = rows // 4
    acc[...] = jnp.zeros_like(acc)

    def edges():
        settle(copies[:4])

        @pl.when(px == 0)
        def _():
            wide[0] = jnp.zeros((modes, cols), F32)
            kappa[pl.ds(0, 8), :] = jnp.zeros((8, cols), F32)

        @pl.when(px == nx - 1)
        def _():
            wide[rows + 1] = jnp.zeros((modes, cols), F32)
            kappa[pl.ds(rows + 8, 8), :] = jnp.zeros((8, cols), F32)

        for i in (0, rows):
            xface[i:i + 1, :] = 0.5 * (kappa[i + 7:i + 8, :] + kappa[i + 8:i + 9, :])
        for i in (0, rows - 1):
            put(1, i, flux(i + 1) - flux(i))

    def build(g, _):
        pl.when(g == 1)(edges)
        starts = [(2 * g + 1) * quarter, lax.rem(2 * g + 2, 4) * quarter]
        for first in starts:
            for s in range(quarter):
                i = first + s
                turn = pltpu.roll(border, (128 - 2 * i) & 127, 1)
                b = [back[i, :, tile(t)] for t in range(tiles)]
                y = [flow[i, :, tile(t)] - jnp.where(lanes == 0, b[t - 1], b[t]) for t in range(tiles)]
                y[0] = y[0] + jnp.where(lanes == 0, turn, 0.0)
                y[-1] = y[-1] + jnp.where(lanes == 127, turn, 0.0)
                put(2, i, jnp.concatenate(y, 1))
        for first in starts:
            at = pl.ds(pl.multiple_of(first * cols, quarter * cols), quarter * cols)
            acc[...] += lax.dot_general(
                m_ref[:, at], m_ref[:columns, at], (((1,), (1,)), ((), ())), preferred_element_type=F32
            )
        return 0

    lax.fori_loop(0, 2, build, 0)
    half = columns // 2
    cross = acc[columns:]
    scale = 1.0 / (rows * cols * nx * ny)
    upper = (acc[:half] + (cross[:half] + cross[:, :half].T)) * scale
    corner = cross[half:, half:]
    corner = (acc[half:columns, half:] + (corner + corner.T)) * scale
    total = jnp.concatenate([upper, jnp.concatenate([corner[half // 2:], corner[:half // 2]], 1)], 0)
    for j in range(ny):
        part[j] = total[j * share:(j + 1) * share]

    copies = [
        pltpu.make_async_remote_copy(
            src_ref=part.at[lax.rem(py + d, ny)], dst_ref=piece.at[py], send_sem=rs_send.at[d], recv_sem=rs_recv.at[d],
            device_id={"gy": lax.rem(py + d, ny)}, device_id_type=MESH,
        )
        for d in range(1, ny)
    ]
    for copy in copies:
        copy.start()
    piece[py] = part[py]
    for copy in copies:
        copy.wait()
    ring[px] = functools.reduce(jnp.add, [piece[j] for j in range(ny)])

    copies = [
        pltpu.make_async_remote_copy(
            src_ref=ring.at[px], dst_ref=ring.at[px], send_sem=all_send.at[d], recv_sem=all_recv.at[d],
            device_id={"gx": lax.rem(px + d, nx)}, device_id_type=MESH,
        )
        for d in range(1, nx)
    ]
    for copy in copies:
        copy.start()
    for copy in copies:
        copy.wait()
    full[py] = functools.reduce(jnp.add, [ring[j] for j in range(nx)])

    copies = [
        pltpu.make_async_remote_copy(
            src_ref=full.at[py], dst_ref=full.at[py], send_sem=ag_send.at[d], recv_sem=ag_recv.at[d],
            device_id={"gy": lax.rem(py + d, ny)}, device_id_type=MESH,
        )
        for d in range(1, ny)
    ]
    for copy in copies:
        copy.start()
    for copy in copies:
        copy.wait()
    whole = jnp.concatenate([full[j] for j in range(ny)], 0)
    upper = whole[:half]
    corner = jnp.concatenate([whole[half:, half:], whole[half:, :half]], 0)
    g_ref[:half, :] = upper
    g_ref[half:, :] = jnp.concatenate([upper[:, half:].T, corner], 1)


def gram(fields, conduct, potential, nx, ny):
    modes, rows, cols = fields.shape
    columns = 4 * modes
    share = 3 * columns // 4 // ny
    vmem = pl.BlockSpec(memory_space=pltpu.VMEM)
    dma = pltpu.SemaphoreType.DMA
    return pl.pallas_call(
        functools.partial(gram_kernel, nx, ny),
        out_shape=(
            pltpu.VMEM((2 * columns, rows * cols), BF16),
            pltpu.VMEM((columns, columns), F32),
        ),
        in_specs=[pl.BlockSpec(memory_space=pltpu.HBM)] * 3,
        out_specs=(vmem, vmem),
        scratch_shapes=[
            pltpu.VMEM((rows + 2, modes, cols), F32),
            pltpu.VMEM((rows + 16, cols), F32),
            pltpu.VMEM((rows, cols), F32),
            pltpu.VMEM((rows + 8, cols), F32),
            pltpu.VMEM((rows, cols), F32),
            pltpu.VMEM((modes + 8, 128), F32),
            pltpu.VMEM((2, modes + 8, 128), F32),
            pltpu.VMEM((rows, modes, cols), F32),
            pltpu.VMEM((rows, modes, cols), F32),
            pltpu.VMEM((rows, modes, cols), F32),
            pltpu.VMEM((2 * columns, columns), F32),
            pltpu.VMEM((ny, share, columns), F32),
            pltpu.VMEM((ny, share, columns), F32),
            pltpu.VMEM((nx, share, columns), F32),
            pltpu.VMEM((ny, share, columns), F32),
            dma((rows + 2,)),
            dma((6,)), dma((6,)), dma((ny,)), dma((ny,)), dma((nx,)), dma((nx,)), dma((ny,)), dma((ny,)),
        ],
        compiler_params=pltpu.CompilerParams(
            collective_id=0, has_side_effects=True, vmem_limit_bytes=28 * 1024 * 1024
        ),
        name="gram",
    )(*(pltpu.with_memory_space_constraint(a, pltpu.HBM) for a in (fields, conduct, potential)))


def factor(g_ref, r_ref, w_ref):
    size = g_ref.shape[0]
    block, width = 8, 16
    parts, tiles = width // block, size // block
    lane = lax.broadcasted_iota(jnp.int32, (block, size), 1)
    sub = lax.broadcasted_iota(jnp.int32, (block, size), 0)

    def row(value, j):
        return jnp.broadcast_to(value[j:j + 1], (block, size))

    def column(value, j):
        return jnp.broadcast_to(value[:, j:j + 1], (block, size))

    z = [g_ref[i * block:(i + 1) * block, :] for i in range(tiles)]
    for at in range(0, size, width):
        if at == size // 2:
            yield
        start = at // block
        stop = start + parts
        inside = (lane >= at) & (lane < at + width)
        cols = [[column(value, at + k) for value in z[start:stop]] for k in range(width)]
        plain = z[start:stop]
        swept = [
            jnp.where(inside, jnp.where(lane == at + h * block + sub, 1.0, 0.0), value)
            for h, value in enumerate(plain)
        ]
        solved = [jnp.zeros((block, size), F32)] * parts
        upper = list(solved)
        for j in range(width):
            h, s = divmod(j, block)
            root = lax.rsqrt(row(cols[j][h], s))
            low = [value * root for value in cols[j]]
            both = list(low)
            both[h] = jnp.where(sub == s, -root, low[h])

            def sweep(values, line):
                return [
                    (jnp.where(sub == s, 0.0, value) if q == h else value) - both[q] * line
                    for q, value in enumerate(values)
                ]

            for k in range(j + 1, width):
                cols[k] = sweep(cols[k], row(low[k // block], k % block))
            line = row(swept[h], s) * root
            solved[h] = jnp.where(sub == s, line, solved[h])
            swept = sweep(swept, line)
            line = row(plain[h], s) * root
            upper[h] = jnp.where(sub == s, line, upper[h])
            plain = [value if q < h else value - low[q] * line for q, value in enumerate(plain)]
            if at >= size // 2:
                yield
        for h in range(parts):
            first = at + h * block
            r_ref[first:first + block, :] = jnp.where(lane >= first + sub, upper[h], 0.0)
            w_ref[first:first + block, :] = jnp.where(lane <= first + sub, solved[h], 0.0)
        for i in range(stop, min(stop + parts, tiles)):
            terms = [column(z[i], at + k) * row(swept[k // block], k % block) for k in range(width)]
            while len(terms) > 1:
                terms = [x + y for x, y in zip(terms[::2], terms[1::2])]
            z[i] = jnp.where(inside, 0.0, z[i]) - terms[0]
        if stop + parts < tiles:
            pads = [jnp.zeros((at, size), F32)] * (at > 0)
            sides = jnp.concatenate(pads + swept + [jnp.zeros((size - at - width, size), F32)], 0)
            change = jnp.dot(
                jnp.concatenate(z[stop + parts:], 0), sides,
                preferred_element_type=F32, precision=lax.Precision.HIGHEST,
            )
            for n, i in enumerate(range(stop + parts, tiles)):
                z[i] = jnp.where(inside, 0.0, z[i]) - change[n * block:(n + 1) * block]
    yield


def apply_kernel(g_ref, m_ref, o_hbm, r_hbm, r_ref, w_ref, upper, lower, out, sent, kept):
    rows, columns, cols = out.shape
    half = columns // 2
    group = 16
    steps = factor(g_ref, r_ref, w_ref)

    def send(side, i):
        part = pl.ds(side * half, half)
        return pltpu.make_async_copy(out.at[i, part], o_hbm.at[part, i, :], sent)

    def over(side, value, groups, between=None):
        first = 0
        for size in groups:
            for i in range(first, first + size):
                out[i, side * half:(side + 1) * half, :] = value(slice(i * cols, (i + 1) * cols))
                if between:
                    between(i)
            for i in range(first, first + size):
                send(side, i).start()
            first += size

    next(steps)
    high, low = split(w_ref[:half, :])
    upper[...] = jnp.concatenate([high[:, :half], high[:, :half], low[:, :half]], 1)

    def first(at):
        near = m_ref[:half, at]
        right = jnp.concatenate([near, m_ref[columns:columns + half, at], near], 0)
        return jnp.dot(upper[...], right, preferred_element_type=F32)

    def advance(i):
        if i >= rows // 2:
            next(steps)
            next(steps)

    over(0, first, (rows // 2, rows // 2), advance)
    for _ in steps:
        pass
    keep = pltpu.make_async_copy(r_ref, r_hbm, kept)
    keep.start()
    high, low = split(w_ref[half:, :])
    lower[:half, :columns] = high
    lower[:half, columns:] = high
    lower[half:, :columns] = low
    lower[half:, columns:] = jnp.zeros_like(low)

    def second(at):
        both = jnp.dot(lower[...], m_ref[:, at], preferred_element_type=F32)
        return both[:half] + both[half:]

    over(1, second, (rows // 2, rows // 4, rows // 4))

    keep.wait()
    pltpu.make_async_copy(out, out, sent).wait()


def apply(total, matrix, rows, cols):
    columns = total.shape[0]
    vmem = pl.BlockSpec(memory_space=pltpu.VMEM)
    return pl.pallas_call(
        apply_kernel,
        out_shape=(
            jax.ShapeDtypeStruct((columns, rows, cols), F32),
            jax.ShapeDtypeStruct((columns, columns), F32),
        ),
        in_specs=[vmem, vmem],
        out_specs=(pl.BlockSpec(memory_space=pltpu.HBM),) * 2,
        scratch_shapes=[
            pltpu.VMEM((columns, columns), F32),
            pltpu.VMEM((columns, columns), F32),
            pltpu.VMEM((columns // 2, 3 * columns // 2), BF16),
            pltpu.VMEM((columns, 2 * columns), BF16),
            pltpu.VMEM((rows, columns, cols), F32),
            pltpu.SemaphoreType.DMA,
            pltpu.SemaphoreType.DMA,
        ],
        compiler_params=pltpu.CompilerParams(vmem_limit_bytes=20 * 1024 * 1024),
        name="apply",
    )(total, pltpu.with_memory_space_constraint(matrix, pltpu.VMEM))


def on_device(nx, ny, mode_fields, conductance, potential):
    _, rows, cols = mode_fields.shape
    matrix, total = gram(mode_fields, conductance, potential, nx, ny)
    return apply(total, matrix, rows, cols)


def solution(mesh):
    placed = (P(None, "gx", "gy"), P("gx", "gy"), P("gx", "gy"))
    return jax.shard_map(
        functools.partial(on_device, mesh.shape["gx"], mesh.shape["gy"]),
        mesh=mesh, in_specs=placed, out_specs=(P(None, "gx", "gy"), P()), check_vma=False,
    )
```

```python
import functools

import jax
import jax.numpy as jnp
from jax import lax
from jax.experimental import pallas as pl
from jax.experimental.pallas import tpu as pltpu
from jax.sharding import PartitionSpec as P

MESH = pl.DeviceIdType.MESH
F32 = jnp.float32
BF16 = jnp.bfloat16


def split(value):
    high = value.astype(BF16)
    return high, (value - high.astype(F32)).astype(BF16)


def gram_kernel(
    nx, ny, u_hbm, k_hbm, p_hbm, m_ref, g_ref,
    wide, kappa, p_ref, xface, yface, edge, halo, turned, flow, back, acc, part, piece, ring, full,
    load, halo_send, halo_recv, rs_send, rs_recv, all_send, all_recv, ag_send, ag_recv,
):
    rows, cols = k_hbm.shape
    modes = u_hbm.shape[0]
    tiles = cols // 128
    columns = 4 * modes
    share = 3 * columns // 4 // ny
    px, py = lax.axis_index("gx"), lax.axis_index("gy")

    def fetch(i):
        return pltpu.make_async_copy(u_hbm.at[:, i, :], wide.at[i + 1], load.at[i])

    own = pl.ds(8, rows)
    load_k = pltpu.make_async_copy(k_hbm, kappa.at[own], load.at[rows])
    load_p = pltpu.make_async_copy(p_hbm, p_ref, load.at[rows + 1])

    load_k.start()
    for i in range(rows // 2):
        fetch(i).start()
    barrier = pltpu.get_barrier_semaphore()
    for d in range(1, nx):
        pl.semaphore_signal(barrier, inc=1, device_id={"gx": lax.rem(px + d, nx)}, device_id_type=MESH)
    for d in range(1, ny):
        pl.semaphore_signal(barrier, inc=1, device_id={"gy": lax.rem(py + d, ny)}, device_id_type=MESH)
    for i in range(rows // 2, rows):
        fetch(i).start()
    load_p.start()

    def iota(height):
        return lax.broadcasted_iota(jnp.int32, (height, 128), 1)

    lanes = iota(modes)
    packed = iota(modes + 8)
    holder = ((packed + 1) & 127) >> 1
    load_k.wait()

    def collect(q, pack):
        for s in range(16):
            fetch(q * 16 + s).wait()
        for s in range(16):
            i = q * 16 + s
            k_row = jnp.broadcast_to(kappa[pl.ds(i + 8, 1), :], (8, cols))
            first = jnp.concatenate([wide[i + 1, :, :128], k_row[:, :128]], 0)
            last = jnp.concatenate([wide[i + 1, :, cols - 128:], k_row[:, cols - 128:]], 0)
            pack = jnp.where(holder == i, pltpu.roll(jnp.where(packed == 0, first, last), 2 * i, 1), pack)
        return pack

    edge[...] = lax.fori_loop(0, rows // 16, collect, jnp.zeros((modes + 8, 128), F32))

    pl.semaphore_wait(barrier, nx + ny - 2)
    has_up, has_down, has_left, has_right = px > 0, px < nx - 1, py > 0, py < ny - 1
    down, up = {"gx": lax.rem(px + 1, nx)}, {"gx": lax.rem(px + nx - 1, nx)}
    right, left = {"gy": lax.rem(py + 1, ny)}, {"gy": lax.rem(py + ny - 1, ny)}
    moves = (
        (wide.at[rows], wide.at[0], down, has_down, has_up),
        (kappa.at[pl.ds(rows, 8)], kappa.at[pl.ds(0, 8)], down, has_down, has_up),
        (wide.at[1], wide.at[rows + 1], up, has_up, has_down),
        (kappa.at[pl.ds(8, 8)], kappa.at[pl.ds(rows + 8, 8)], up, has_up, has_down),
        (edge, halo.at[0], right, has_right, has_left),
        (edge, halo.at[1], left, has_left, has_right),
    )
    copies = [
        (
            pltpu.make_async_remote_copy(
                src_ref=src, dst_ref=dst, send_sem=halo_send.at[n], recv_sem=halo_recv.at[n],
                device_id=device, device_id_type=MESH,
            ), sends, receives,
        )
        for n, (src, dst, device, sends, receives) in enumerate(moves)
    ]
    for copy, sends, _ in copies:
        @pl.when(sends)
        def _():
            copy.start()

    def put(block, i, value):
        high, low = split(value)
        at = slice(i * cols, (i + 1) * cols) if isinstance(i, int) else pl.ds(pl.multiple_of(i * cols, cols), cols)
        m_ref[block * modes:(block + 1) * modes, at] = high
        m_ref[columns + block * modes:columns + (block + 1) * modes, at] = low

    def flux(i):
        return xface[pl.ds(i, 1), :] * (wide[i] - wide[i + 1])

    xface[pl.ds(1, rows - 1), :] = 0.5 * (kappa[pl.ds(8, rows - 1), :] + kappa[pl.ds(9, rows - 1), :])
    lane = iota(rows)

    def tile(t):
        return slice(t * 128, (t + 1) * 128)

    k_tile = [kappa[own, t * 128:(t + 1) * 128] for t in range(tiles)]
    k_next = [pltpu.roll(k, 127, 1) for k in k_tile]
    for t in range(tiles):
        face = 0.5 * (k_tile[t] + (jnp.where(lane == 127, k_next[t + 1], k_next[t]) if t + 1 < tiles else k_next[t]))
        yface[:, t * 128:(t + 1) * 128] = face if t + 1 < tiles else jnp.where(lane == 127, 0.0, face)
    load_p.wait()

    def local(i):
        center = wide[i + 1]
        put(0, i, center)
        put(3, i, p_ref[pl.ds(i, 1), :] * center)
        for t in range(tiles):
            turned[i, :, tile(t)] = pltpu.roll(center[:, tile(t)], 127, 1)

    def stream(g, _):
        for s in range(group):
            i = g * group + s
            scale = yface[pl.ds(i, 1), :]
            r = [turned[i, :, tile(t)] for t in range(tiles)]
            for t in range(tiles):
                after = jnp.where(lanes == 127, r[t + 1], r[t]) if t + 1 < tiles else r[t]
                f = scale[:, tile(t)] * (wide[i + 1, :, tile(t)] - after)
                flow[i, :, tile(t)] = f
                back[i, :, tile(t)] = pltpu.roll(f, 1, 1)
        return 0

    group = 32

    def inner(first, count, before):
        for s in range(group):
            local(first + s)
            if s < count:
                after = flux(first + s + 2)
                put(1, first + s + 1, after - before)
                before = after
        return before

    def sweep(g, before):
        return inner(g * group, group, before)

    inner(rows - group, group - 2, lax.fori_loop(0, rows // group - 1, sweep, flux(1)))
    lax.fori_loop(0, rows // group, stream, 0)

    def settle(some):
        for copy, sends, receives in some:
            @pl.when(sends)
            def _():
                copy.wait_send()

            @pl.when(receives)
            def _():
                copy.wait_recv()

    settle(copies[4:])

    @pl.when(py == 0)
    def _():
        halo[0] = jnp.zeros((modes + 8, 128), F32)

    @pl.when(py == ny - 1)
    def _():
        halo[1] = jnp.zeros((modes + 8, 128), F32)

    mine = edge[...]
    other = jnp.where((packed & 1) == 0, pltpu.roll(halo[0], 1, 1), pltpu.roll(halo[1], 127, 1))
    border = 0.5 * (mine[modes:modes + 1] + other[modes:modes + 1]) * (mine[:modes] - other[:modes])

    quarter = rows // 4
    acc[...] = jnp.zeros_like(acc)

    def edges():
        settle(copies[:4])

        @pl.when(px == 0)
        def _():
            wide[0] = jnp.zeros((modes, cols), F32)
            kappa[pl.ds(0, 8), :] = jnp.zeros((8, cols), F32)

        @pl.when(px == nx - 1)
        def _():
            wide[rows + 1] = jnp.zeros((modes, cols), F32)
            kappa[pl.ds(rows + 8, 8), :] = jnp.zeros((8, cols), F32)

        for i in (0, rows):
            xface[i:i + 1, :] = 0.5 * (kappa[i + 7:i + 8, :] + kappa[i + 8:i + 9, :])
        for i in (0, rows - 1):
            put(1, i, flux(i + 1) - flux(i))

    def build(g, _):
        pl.when(g == 1)(edges)
        starts = [(2 * g + 1) * quarter, lax.rem(2 * g + 2, 4) * quarter]
        for first in starts:
            for s in range(quarter):
                i = first + s
                turn = pltpu.roll(border, (128 - 2 * i) & 127, 1)
                b = [back[i, :, tile(t)] for t in range(tiles)]
                y = [flow[i, :, tile(t)] - jnp.where(lanes == 0, b[t - 1], b[t]) for t in range(tiles)]
                y[0] = y[0] + jnp.where(lanes == 0, turn, 0.0)
                y[-1] = y[-1] + jnp.where(lanes == 127, turn, 0.0)
                put(2, i, jnp.concatenate(y, 1))
        for first in starts:
            at = pl.ds(pl.multiple_of(first * cols, quarter * cols), quarter * cols)
            acc[...] += lax.dot_general(
                m_ref[:, at], m_ref[:columns, at], (((1,), (1,)), ((), ())), preferred_element_type=F32
            )
        return 0

    lax.fori_loop(0, 2, build, 0)
    half = columns // 2
    cross = acc[columns:]
    scale = 1.0 / (rows * cols * nx * ny)
    upper = (acc[:half] + (cross[:half] + cross[:, :half].T)) * scale
    corner = cross[half:, half:]
    corner = (acc[half:columns, half:] + (corner + corner.T)) * scale
    total = jnp.concatenate([upper, jnp.concatenate([corner[half // 2:], corner[:half // 2]], 1)], 0)
    for j in range(ny):
        part[j] = total[j * share:(j + 1) * share]

    copies = [
        pltpu.make_async_remote_copy(
            src_ref=part.at[lax.rem(py + d, ny)], dst_ref=piece.at[py], send_sem=rs_send.at[d], recv_sem=rs_recv.at[d],
            device_id={"gy": lax.rem(py + d, ny)}, device_id_type=MESH,
        )
        for d in range(1, ny)
    ]
    for copy in copies:
        copy.start()
    piece[py] = part[py]
    for copy in copies:
        copy.wait()
    ring[px] = functools.reduce(jnp.add, [piece[j] for j in range(ny)])

    copies = [
        pltpu.make_async_remote_copy(
            src_ref=ring.at[px], dst_ref=ring.at[px], send_sem=all_send.at[d], recv_sem=all_recv.at[d],
            device_id={"gx": lax.rem(px + d, nx)}, device_id_type=MESH,
        )
        for d in range(1, nx)
    ]
    for copy in copies:
        copy.start()
    for copy in copies:
        copy.wait()
    full[py] = functools.reduce(jnp.add, [ring[j] for j in range(nx)])

    copies = [
        pltpu.make_async_remote_copy(
            src_ref=full.at[py], dst_ref=full.at[py], send_sem=ag_send.at[d], recv_sem=ag_recv.at[d],
            device_id={"gy": lax.rem(py + d, ny)}, device_id_type=MESH,
        )
        for d in range(1, ny)
    ]
    for copy in copies:
        copy.start()
    for copy in copies:
        copy.wait()
    whole = jnp.concatenate([full[j] for j in range(ny)], 0)
    upper = whole[:half]
    corner = jnp.concatenate([whole[half:, half:], whole[half:, :half]], 0)
    g_ref[:half, :] = upper
    g_ref[half:, :] = jnp.concatenate([upper[:, half:].T, corner], 1)


def gram(fields, conduct, potential, nx, ny):
    modes, rows, cols = fields.shape
    columns = 4 * modes
    share = 3 * columns // 4 // ny
    vmem = pl.BlockSpec(memory_space=pltpu.VMEM)
    dma = pltpu.SemaphoreType.DMA
    return pl.pallas_call(
        functools.partial(gram_kernel, nx, ny),
        out_shape=(
            pltpu.VMEM((2 * columns, rows * cols), BF16),
            pltpu.VMEM((columns, columns), F32),
        ),
        in_specs=[pl.BlockSpec(memory_space=pltpu.HBM)] * 3,
        out_specs=(vmem, vmem),
        scratch_shapes=[
            pltpu.VMEM((rows + 2, modes, cols), F32),
            pltpu.VMEM((rows + 16, cols), F32),
            pltpu.VMEM((rows, cols), F32),
            pltpu.VMEM((rows + 8, cols), F32),
            pltpu.VMEM((rows, cols), F32),
            pltpu.VMEM((modes + 8, 128), F32),
            pltpu.VMEM((2, modes + 8, 128), F32),
            pltpu.VMEM((rows, modes, cols), F32),
            pltpu.VMEM((rows, modes, cols), F32),
            pltpu.VMEM((rows, modes, cols), F32),
            pltpu.VMEM((2 * columns, columns), F32),
            pltpu.VMEM((ny, share, columns), F32),
            pltpu.VMEM((ny, share, columns), F32),
            pltpu.VMEM((nx, share, columns), F32),
            pltpu.VMEM((ny, share, columns), F32),
            dma((rows + 2,)),
            dma((6,)), dma((6,)), dma((ny,)), dma((ny,)), dma((nx,)), dma((nx,)), dma((ny,)), dma((ny,)),
        ],
        compiler_params=pltpu.CompilerParams(
            collective_id=0, has_side_effects=True, vmem_limit_bytes=28 * 1024 * 1024
        ),
        name="gram",
    )(*(pltpu.with_memory_space_constraint(a, pltpu.HBM) for a in (fields, conduct, potential)))


def factor(g_ref, r_ref, w_ref):
    size = g_ref.shape[0]
    block, width = 8, 16
    parts, tiles = width // block, size // block
    lane = lax.broadcasted_iota(jnp.int32, (block, size), 1)
    sub = lax.broadcasted_iota(jnp.int32, (block, size), 0)

    def row(value, j):
        return jnp.broadcast_to(value[j:j + 1], (block, size))

    def column(value, j):
        return jnp.broadcast_to(value[:, j:j + 1], (block, size))

    z = [g_ref[i * block:(i + 1) * block, :] for i in range(tiles)]
    for at in range(0, size, width):
        if at == size // 2:
            yield
        start = at // block
        stop = start + parts
        inside = (lane >= at) & (lane < at + width)
        cols = [[column(value, at + k) for value in z[start:stop]] for k in range(width)]
        plain = z[start:stop]
        swept = [
            jnp.where(inside, jnp.where(lane == at + h * block + sub, 1.0, 0.0), value)
            for h, value in enumerate(plain)
        ]
        solved = [jnp.zeros((block, size), F32)] * parts
        upper = list(solved)
        for j in range(width):
            h, s = divmod(j, block)
            root = lax.rsqrt(row(cols[j][h], s))
            low = [value * root for value in cols[j]]
            both = list(low)
            both[h] = jnp.where(sub == s, -root, low[h])

            def sweep(values, line):
                return [
                    (jnp.where(sub == s, 0.0, value) if q == h else value) - both[q] * line
                    for q, value in enumerate(values)
                ]

            for k in range(j + 1, width):
                cols[k] = sweep(cols[k], row(low[k // block], k % block))
            line = row(swept[h], s) * root
            solved[h] = jnp.where(sub == s, line, solved[h])
            swept = sweep(swept, line)
            line = row(plain[h], s) * root
            upper[h] = jnp.where(sub == s, line, upper[h])
            plain = [value if q < h else value - low[q] * line for q, value in enumerate(plain)]
            if at >= size // 2:
                yield
        for h in range(parts):
            first = at + h * block
            r_ref[first:first + block, :] = jnp.where(lane >= first + sub, upper[h], 0.0)
            w_ref[first:first + block, :] = jnp.where(lane <= first + sub, solved[h], 0.0)
        for i in range(stop, min(stop + parts, tiles)):
            terms = [column(z[i], at + k) * row(swept[k // block], k % block) for k in range(width)]
            while len(terms) > 1:
                terms = [x + y for x, y in zip(terms[::2], terms[1::2])]
            z[i] = jnp.where(inside, 0.0, z[i]) - terms[0]
        if stop + parts < tiles:
            pads = [jnp.zeros((at, size), F32)] * (at > 0)
            sides = jnp.concatenate(pads + swept + [jnp.zeros((size - at - width, size), F32)], 0)
            change = jnp.dot(
                jnp.concatenate(z[stop + parts:], 0), sides,
                preferred_element_type=F32, precision=lax.Precision.HIGHEST,
            )
            for n, i in enumerate(range(stop + parts, tiles)):
                z[i] = jnp.where(inside, 0.0, z[i]) - change[n * block:(n + 1) * block]
    yield


def apply_kernel(g_ref, m_ref, o_hbm, r_hbm, r_ref, w_ref, upper, lower, out, sent, kept):
    rows, columns, cols = out.shape
    half = columns // 2
    group = 16
    steps = factor(g_ref, r_ref, w_ref)

    def send(side, i):
        part = pl.ds(side * half, half)
        return pltpu.make_async_copy(out.at[i, part], o_hbm.at[part, i, :], sent)

    def over(side, value, groups, between=None):
        first = 0
        for size in groups:
            for i in range(first, first + size):
                out[i, side * half:(side + 1) * half, :] = value(slice(i * cols, (i + 1) * cols))
                if between:
                    between(i)
            for i in range(first, first + size):
                send(side, i).start()
            first += size

    next(steps)
    high, low = split(w_ref[:half, :])
    upper[...] = jnp.concatenate([high[:, :half], high[:, :half], low[:, :half]], 1)

    def first(at):
        near = m_ref[:half, at]
        right = jnp.concatenate([near, m_ref[columns:columns + half, at], near], 0)
        return jnp.dot(upper[...], right, preferred_element_type=F32)

    def advance(i):
        if i >= rows // 2:
            next(steps)
            next(steps)

    over(0, first, (rows // 2, rows // 2), advance)
    for _ in steps:
        pass
    keep = pltpu.make_async_copy(r_ref, r_hbm, kept)
    keep.start()
    high, low = split(w_ref[half:, :])
    lower[:half, :columns] = high
    lower[:half, columns:] = high
    lower[half:, :columns] = low
    lower[half:, columns:] = jnp.zeros_like(low)

    def second(at):
        both = jnp.dot(lower[...], m_ref[:, at], preferred_element_type=F32)
        return both[:half] + both[half:]

    over(1, second, (rows // 4, rows // 2, rows // 4))

    keep.wait()
    pltpu.make_async_copy(out, out, sent).wait()


def apply(total, matrix, rows, cols):
    columns = total.shape[0]
    vmem = pl.BlockSpec(memory_space=pltpu.VMEM)
    return pl.pallas_call(
        apply_kernel,
        out_shape=(
            jax.ShapeDtypeStruct((columns, rows, cols), F32),
            jax.ShapeDtypeStruct((columns, columns), F32),
        ),
        in_specs=[vmem, vmem],
        out_specs=(pl.BlockSpec(memory_space=pltpu.HBM),) * 2,
        scratch_shapes=[
            pltpu.VMEM((columns, columns), F32),
            pltpu.VMEM((columns, columns), F32),
            pltpu.VMEM((columns // 2, 3 * columns // 2), BF16),
            pltpu.VMEM((columns, 2 * columns), BF16),
            pltpu.VMEM((rows, columns, cols), F32),
            pltpu.SemaphoreType.DMA,
            pltpu.SemaphoreType.DMA,
        ],
        compiler_params=pltpu.CompilerParams(vmem_limit_bytes=20 * 1024 * 1024),
        name="apply",
    )(total, pltpu.with_memory_space_constraint(matrix, pltpu.VMEM))


def on_device(nx, ny, mode_fields, conductance, potential):
    _, rows, cols = mode_fields.shape
    matrix, total = gram(mode_fields, conductance, potential, nx, ny)
    return apply(total, matrix, rows, cols)


def solution(mesh):
    placed = (P(None, "gx", "gy"), P("gx", "gy"), P("gx", "gy"))
    return jax.shard_map(
        functools.partial(on_device, mesh.shape["gx"], mesh.shape["gy"]),
        mesh=mesh, in_specs=placed, out_specs=(P(None, "gx", "gy"), P()), check_vma=False,
    )
```
